128 devices in a mesh: section: 16 (over z, x_hi, core), tm: 8 (over y, x_lo).
Axes of the slice: x: 4 (x_hi: 2, x_lo: 2; x = x_hi * 2 + x_lo), y: 4, z: 4, core: 2. Of those that a mesh axis runs over, the one named last changes fastest.
Arguments:
- frames: bfloat16 [4, 512, 1024], P(None, 'tm'), may hold values from -6 to 6, as said below
- lengths: int32 [4], replicated, may hold values from 128 to 512
- ffn_gain: float32 [16, 1024], P('section'), may hold values from 0.1 to 1.9
- ffn_up: bfloat16 [16, 1024, 2048], P('section'), may hold values from -0.1875 to 0.1875
- ffn_down: bfloat16 [16, 2048, 1024], P('section'), may hold values from -0.125 to 0.125
- attn_gain: float32 [16, 1024], P('section'), may hold values from 0.1 to 1.9
- query_weight: bfloat16 [16, 1024, 1024], P('section'), may hold values from -8 to 8
- key_weight: bfloat16 [16, 1024, 1024], P('section'), may hold values from -0.1875 to 0.1875
- value_weight: bfloat16 [16, 1024, 1024], P('section'), may hold values from -0.1875 to 0.1875
- out_weight: bfloat16 [16, 1024, 1024], P('section'), may hold values from -0.1875 to 0.1875
- conv_gain: float32 [16, 1024], P('section'), may hold values from 0.1 to 1.9
- expand_weight: bfloat16 [16, 1024, 2048], P('section'), may hold values from -0.1875 to 0.1875
- depth_weight: float32 [16, 31, 1024], P('section'), may hold values from -1 to 1
- depth_gain: float32 [16, 1024], P('section'), may hold values from 0.1 to 1.9
- norm_shift: float32 [16, 1024], P('section'), may hold values from -0.5 to 0.5
- shrink_weight: bfloat16 [16, 1024, 1024], P('section'), may hold values from -0.1875 to 0.1875
- final_gain: float32 [16, 1024], P('section'), may hold values from 0.1 to 1.9
Outputs:
- hidden_states: bfloat16 [16, 4, 512, 1024], P('section', None, 'tm')
The draws below stay inside these ranges and needn't reach their ends.
Inputs may be any that keep to these rules, and one draw needn't show every extreme that they name: `frames`: input features of order one.
All inputs are finite; a program needn't handle non-finite values.
Results may differ from the reference program's by a relative error of at most 0.02.
Values may be sent and summed in bfloat16 or wider, within the bound.
A program may use at most 128 MiB of HBM per device.

```python
import jax
import jax.numpy as jnp
from jax import lax

D = 1024
HEADS = 16
HEAD = 64
KERNEL = 31
FF = 2048
MICRO = 4
SECTIONS = 16
LEN = 512


def shared_projection(key):
    base = jax.random.normal(jax.random.fold_in(key, 101), (SECTIONS, D, D), jnp.float32) * D ** (-0.5)
    own = jax.random.normal(jax.random.fold_in(key, 102), (SECTIONS, D, D), jnp.float32) * D ** (-0.5)
    base = jnp.clip(base, -6.0 / 32.0, 6.0 / 32.0)
    own = jnp.clip(own, -6.0 / 32.0, 6.0 / 32.0)
    return (base, own)


def draw_key_weight(key, part):
    base, own = shared_projection(key)
    return base.astype(jnp.bfloat16)


def draw_query_weight(key, part):
    base, own = shared_projection(key)
    grades = jax.random.randint(jax.random.fold_in(key, 104), (SECTIONS, HEADS), 0, 4)
    drawn = jnp.where(grades > 0, 0.25 * jnp.exp2(grades.astype(jnp.float32)), 0.0)
    drawn = jnp.repeat(drawn, HEAD, axis=1)[:, None, :]
    result = base * drawn + own
    return jnp.clip(result, -8.0, 8.0).astype(jnp.bfloat16)


def draw_frames(key, part):
    values = jax.random.normal(jax.random.fold_in(key, 201), (MICRO, LEN, D), jnp.float32)
    return jnp.clip(values, -6.0, 6.0).astype(jnp.bfloat16)


def touch_ends(values, stream_key, low, high):
    shape = values.shape
    index_at = [jax.random.randint(jax.random.fold_in(stream_key, axis), (), 0, shape[axis]) for axis in range(len(shape))]
    values = values.at[tuple(index_at)].set(low)
    longest = shape.index(max(shape))
    index_at[longest] = (index_at[longest] + 1) % shape[longest]
    return values.at[tuple(index_at)].set(high)


def steps_of(own_key, extent, split, least, high):
    def one(axis_at, shards_of):
        draws = jax.random.uniform(jax.random.fold_in(jax.random.fold_in(own_key, 6), axis_at), (shards_of,), jnp.float32, least / len(split), high / len(split))
        return jnp.repeat(jnp.exp(draws), extent[axis_at] // shards_of).reshape((-1,) + (1,) * (len(extent) - axis_at - 1))

    factor_of = one(*split[0])
    for cut in split[1:]:
        factor_of = factor_of * one(*cut)
    return factor_of


def normal_values(stream_key, extent, deviation, limit, split=(), kind=jnp.bfloat16):
    values = deviation * jax.random.normal(stream_key, extent, jnp.float32)
    if split:
        values = values * steps_of(stream_key, extent, split, -0.22, 0.18)
    return jnp.clip(values, -limit, limit).astype(kind)


def setup_inputs(seed: int = 0) -> dict:
    seeds = jax.random.split(jax.random.key(seed), 18)
    frames = draw_frames(jax.random.fold_in(seeds[17], 71), 0)
    lengths = touch_ends(jax.random.randint(seeds[1], (MICRO,), LEN // 4, LEN + 1), jax.random.fold_in(seeds[1], 1), LEN // 4, LEN).astype(jnp.int32)
    ffn_gain = jnp.clip(1.0 + 0.18 * jax.random.normal(seeds[2], (SECTIONS, D), jnp.float32), 0.1, 1.9)
    ffn_up = normal_values(seeds[3], (SECTIONS, D, FF), D ** -0.5, 0.1875, ((0, 16),))
    ffn_down = normal_values(seeds[4], (SECTIONS, FF, D), FF ** -0.5, 0.125, ((0, 16),))
    attn_gain = jnp.clip(1.0 + 0.18 * jax.random.normal(seeds[5], (SECTIONS, D), jnp.float32), 0.1, 1.9)
    query_weight = draw_query_weight(jax.random.fold_in(seeds[17], 71), 0)
    key_weight = draw_key_weight(jax.random.fold_in(seeds[17], 71), 0)
    value_weight = normal_values(seeds[8], (SECTIONS, D, D), D ** -0.5, 0.1875, ((0, 16),))
    out_weight = normal_values(seeds[9], (SECTIONS, D, D), D ** -0.5, 0.1875, ((0, 16),))
    conv_gain = jnp.clip(1.0 + 0.18 * jax.random.normal(seeds[10], (SECTIONS, D), jnp.float32), 0.1, 1.9)
    expand_weight = normal_values(seeds[11], (SECTIONS, D, 2 * D), D ** -0.5, 0.1875, ((0, 16),))
    depth_weight = normal_values(seeds[12], (SECTIONS, KERNEL, D), KERNEL ** -0.5, 1.0, ((0, 16),), jnp.float32)
    depth_gain = jnp.clip(1.0 + 0.18 * jax.random.normal(seeds[13], (SECTIONS, D), jnp.float32), 0.1, 1.9)
    norm_shift = jnp.clip(jax.random.uniform(seeds[14], (SECTIONS, D), jnp.float32, -0.5, 0.5) * steps_of(seeds[14], (SECTIONS, D), ((0, 16),), -0.4, 0.0), -0.5, 0.5)
    shrink_weight = normal_values(seeds[15], (SECTIONS, D, D), D ** -0.5, 0.1875, ((0, 16),))
    final_gain = jnp.clip(1.0 + 0.18 * jax.random.normal(seeds[16], (SECTIONS, D), jnp.float32), 0.1, 1.9)
    return {"frames": frames, "lengths": lengths, "ffn_gain": ffn_gain, "ffn_up": ffn_up, "ffn_down": ffn_down, "attn_gain": attn_gain, "query_weight": query_weight, "key_weight": key_weight, "value_weight": value_weight, "out_weight": out_weight, "conv_gain": conv_gain, "expand_weight": expand_weight, "depth_weight": depth_weight, "depth_gain": depth_gain, "norm_shift": norm_shift, "shrink_weight": shrink_weight, "final_gain": final_gain}


EPS = 1e-05

def normalize(value, gain):
    mean = lax.optimization_barrier(jnp.mean(value, axis=-1, keepdims=True))
    centred = value - mean
    spread = lax.optimization_barrier(jnp.mean(centred * centred, axis=-1, keepdims=True))
    return centred * lax.rsqrt(spread + EPS) * gain

def block(inputs, length, weights):
    ffn_gain, ffn_up, ffn_down, attn_gain, query_weight, key_weight, value_weight, out_weight, conv_gain, expand_weight, depth_weight, depth_gain, norm_shift, shrink_weight, final_gain = weights
    positions = jnp.arange(LEN, dtype=jnp.int32)
    keep = positions < length
    ffn_normed = normalize(inputs.astype(jnp.float32), ffn_gain).astype(jnp.bfloat16)
    inner = jax.nn.silu(jnp.dot(ffn_normed, ffn_up, preferred_element_type=jnp.float32)).astype(jnp.bfloat16)
    start = inputs.astype(jnp.float32) + 0.5 * jnp.dot(inner, ffn_down, preferred_element_type=jnp.float32)
    normed = normalize(start, attn_gain).astype(jnp.bfloat16)
    queries = jnp.dot(normed, query_weight, preferred_element_type=jnp.float32).astype(jnp.bfloat16)
    keys = jnp.dot(normed, key_weight, preferred_element_type=jnp.float32).astype(jnp.bfloat16)
    values = jnp.dot(normed, value_weight, preferred_element_type=jnp.float32).astype(jnp.bfloat16)
    scale = 1.0 / HEAD ** 0.5

    def one_head(index):
        begin = (index * HEAD).astype(jnp.int32)
        q_head = lax.dynamic_slice_in_dim(queries, begin, HEAD, 1)
        k_head = lax.dynamic_slice_in_dim(keys, begin, HEAD, 1)
        v_head = lax.dynamic_slice_in_dim(values, begin, HEAD, 1)
        scores = jnp.dot(q_head, k_head.T, preferred_element_type=jnp.float32) * scale
        scores = jnp.where(keep[None, :], scores, -1e+30)
        peak = lax.optimization_barrier(jnp.max(scores, axis=-1, keepdims=True))
        weights_h = jnp.exp(scores - peak)
        total = lax.optimization_barrier(jnp.sum(weights_h, axis=-1, keepdims=True))
        mixed = jnp.dot(weights_h.astype(jnp.bfloat16), v_head, preferred_element_type=jnp.float32)
        return (mixed / total).astype(jnp.bfloat16)
    per_head = lax.map(one_head, jnp.arange(HEADS, dtype=jnp.int32))
    context = jnp.transpose(per_head, (1, 0, 2)).reshape(LEN, D)
    mid = start + jnp.dot(context, out_weight, preferred_element_type=jnp.float32)
    conv_in = normalize(mid, conv_gain).astype(jnp.bfloat16)
    expanded = jnp.dot(conv_in, expand_weight, preferred_element_type=jnp.float32)
    glu = expanded[:, :D] * jax.nn.sigmoid(expanded[:, D:]) * keep[:, None].astype(jnp.float32)
    glu = glu.astype(jnp.bfloat16)
    rim = KERNEL // 2
    padded = jnp.pad(glu, ((rim, rim), (0, 0))).astype(jnp.float32)
    depth = jnp.zeros((LEN, D), jnp.float32)
    for offset in range(KERNEL):
        depth = depth + padded[offset:offset + LEN] * depth_weight[offset]
    shifted = normalize(depth, depth_gain) + norm_shift
    swished = (shifted * jax.nn.sigmoid(shifted)).astype(jnp.bfloat16)
    closing = mid + jnp.dot(swished, shrink_weight, preferred_element_type=jnp.float32)
    return normalize(closing, final_gain).astype(jnp.bfloat16)

def reference(frames, lengths, ffn_gain, ffn_up, ffn_down, attn_gain, query_weight, key_weight, value_weight, out_weight, conv_gain, expand_weight, depth_weight, depth_gain, norm_shift, shrink_weight, final_gain):
    stacked = (ffn_gain, ffn_up, ffn_down, attn_gain, query_weight, key_weight, value_weight, out_weight, conv_gain, expand_weight, depth_weight, depth_gain, norm_shift, shrink_weight, final_gain)

    def section_step(current, weights):
        result = lax.map(lambda pair: block(pair[0], pair[1], weights), (current, lengths))
        return (result, result)
    finished, hidden_states = lax.scan(section_step, frames, stacked)
    return hidden_states
```

```python
import functools

import jax
import jax.numpy as jnp
from jax import lax
from jax.experimental import pallas as pl
from jax.experimental.pallas import tpu as pltpu
from jax.sharding import PartitionSpec as P

MESH = pl.DeviceIdType.MESH
F32 = jnp.float32
BF16 = jnp.bfloat16
EPS = 1e-05
D = 1024
FF = 2048
HEADS = 16
ROWS = 256
LEN = 512
TAPS = 31
UTTS = 4
STAGES = 8
PIECE = 64
PIECES = ROWS // PIECE
SHAPES = ((D, FF), (FF, D), (D, D), (D, D), (D, D), (D, D), (D, 2 * D), (D, D))


def sigmoid(v):
    return 0.5 * jnp.tanh(0.5 * v) + 0.5


def normed(v, gain):
    mean = jnp.mean(v, axis=-1, keepdims=True)
    centred = v - mean
    spread = jnp.mean(centred * centred, axis=-1, keepdims=True)
    return centred * lax.rsqrt(spread + EPS) * gain


def dot(a, b):
    return jnp.dot(a, b, preferred_element_type=F32)


def block_kernel(
    lengths,
    frames,
    ffn_gain,
    attn_gain,
    conv_gain,
    depth_gain,
    norm_shift,
    final_gain,
    depth_weight,
    h_up,
    h_down,
    h_key,
    h_value,
    h_query,
    h_out,
    h_expand,
    h_shrink,
    out,
    w_up,
    w_down,
    w_key,
    w_value,
    w_query,
    w_out,
    w_expand,
    w_shrink,
    vec,
    taps,
    xs,
    act,
    wide,
    res,
    kv,
    rim_out,
    rim_in,
    padded,
    depth,
    local_sem,
    push_sem,
    pull_sem,
    x_send,
    x_recv,
    out_send,
    out_recv,
    kv_send,
    kv_recv,
    rim_send,
    rim_recv,
    frame_send,
):
    s = lax.axis_index("section")
    t = lax.axis_index("tm")
    k = s // 2
    c = lax.rem(s, 2)
    u = t // 2
    side = 1 - lax.rem(k, 2)
    active = lax.rem(t, 2) == side
    partner = {"section": 2 * k + 1 - c, "tm": t}
    here = {"section": s, "tm": t}
    del here

    hbm = (h_up, h_down, h_key, h_value, h_query, h_out, h_expand, h_shrink)
    vmem = (w_up, w_down, w_key, w_value, w_query, w_out, w_expand, w_shrink)
    small = (ffn_gain, attn_gain, conv_gain, depth_gain, norm_shift, final_gain)

    def sources():
        pairs = [(small[i], vec.at[c, i]) for i in range(6)]
        pairs += [(depth_weight.at[0], taps.at[c])]
        pairs += [(hbm[i].at[0], vmem[i].at[c]) for i in range(8)]
        return pairs

    def arrivals(slot):
        refs = [vec.at[slot, i] for i in range(6)] + [taps.at[slot]]
        return refs + [vmem[i].at[slot] for i in range(8)]

    def local(i):
        src, dst = sources()[i]
        return pltpu.make_async_copy(src, dst, local_sem.at[i])

    def push(i):
        src, dst = sources()[i]
        return pltpu.make_async_remote_copy(
            src, dst, push_sem.at[i], pull_sem.at[i], device_id=partner, device_id_type=MESH
        )

    def pull(i, slot):
        ref = arrivals(slot)[i]
        return pltpu.make_async_remote_copy(
            ref, ref, push_sem.at[i], pull_sem.at[i], device_id=partner, device_id_type=MESH
        )

    ORDER = (0, 7, 8, 1, 9, 10, 11, 12, 2, 13, 3, 4, 6, 14, 5)

    @pl.when(active)
    def _():
        for i in ORDER:
            local(i).start()
        for i in ORDER:
            push(i).start()

    def frame_copy(v):
        return pltpu.make_async_remote_copy(
            frames.at[v],
            xs.at[0, pl.ds(pl.multiple_of(lax.rem(t, 4) * PIECE, PIECE), PIECE)],
            frame_send.at[v],
            x_recv.at[lax.rem(t, 4)],
            device_id={"section": s, "tm": 2 * v + 1},
            device_id_type=MESH,
        )

    def frame_local(v):
        return pltpu.make_async_copy(
            frames.at[v],
            xs.at[0, pl.ds(pl.multiple_of(lax.rem(t, 4) * PIECE, PIECE), PIECE)],
            x_recv.at[lax.rem(t, 4)],
        )

    sends_frames = (k == 0) & (t // 4 == c)
    for v in range(UTTS):

        @pl.when(sends_frames & (t != 2 * v + 1))
        def _(v=v):
            frame_copy(v).start()

        @pl.when(sends_frames & (t == 2 * v + 1))
        def _(v=v):
            frame_local(v).start()

    def piece_rows(j):
        return pl.ds(j * PIECE, PIECE)

    def forward(j):
        return pltpu.make_async_remote_copy(
            xs.at[2, piece_rows(j)],
            xs.at[0, piece_rows(j)],
            x_send.at[j],
            x_recv.at[j],
            device_id={"section": lax.rem(s + 2, 16), "tm": 2 * u + 1 - side},
            device_id_type=MESH,
        )

    def scatter(slot, j):
        return pltpu.make_async_remote_copy(
            xs.at[slot + 1, piece_rows(j)],
            out.at[0, u],
            out_send.at[slot, j],
            out_recv.at[u],
            device_id={"section": 2 * k + slot, "tm": 4 * c + j},
            device_id_type=MESH,
        )

    def scatter_local(slot, j):
        return pltpu.make_async_copy(xs.at[slot + 1, piece_rows(j)], out.at[0, u], out_recv.at[u])

    def own_piece(slot, j):
        return (slot == c) & (4 * c + j == t)

    own = pl.ds(pl.multiple_of(c * ROWS, ROWS), ROWS)

    def kv_copy(slot, i):
        return pltpu.make_async_remote_copy(
            kv.at[slot, i, own],
            kv.at[slot, i, own],
            kv_send.at[slot, i],
            kv_recv.at[slot, i],
            device_id=partner,
            device_id_type=MESH,
        )

    def kv_arrival(slot, i):
        other = pl.ds(pl.multiple_of((1 - c) * ROWS, ROWS), ROWS)
        return pltpu.make_async_remote_copy(
            kv.at[slot, i, other],
            kv.at[slot, i, other],
            kv_send.at[slot, i],
            kv_recv.at[slot, i],
            device_id=partner,
            device_id_type=MESH,
        )

    def rim_copy(slot):
        return pltpu.make_async_remote_copy(
            rim_out.at[slot],
            rim_in.at[slot],
            rim_send.at[slot],
            rim_recv.at[slot],
            device_id=partner,
            device_id_type=MESH,
        )

    def run_slot(slot, carry):
        mine = slot == c

        def ready(*ids):
            for i in ids:

                @pl.when(mine)
                def _(i=i):
                    local(i).wait()

                @pl.when(jnp.logical_not(mine))
                def _(i=i):
                    pull(i, slot).wait_recv()

        length = lengths[u]

        @pl.when(slot == 0)
        def _():
            for j in range(PIECES):
                itself = (k == 0) & (4 * c + j == t)

                @pl.when(itself)
                def _():
                    for v in range(UTTS):

                        @pl.when(t == 2 * v + 1)
                        def _(v=v):
                            frame_local(v).wait()

                @pl.when(jnp.logical_not(itself))
                def _(j=j):
                    forward(j).wait_recv()

        ready(0, 7)
        act[...] = normed(xs[slot].astype(F32), vec[slot, 0]).astype(BF16)

        def up_tile(n, carry):
            cols = pl.ds(pl.multiple_of(n * 512, 512), 512)
            v = dot(act[...], w_up[slot, :, cols])
            wide[:, cols] = (v * sigmoid(v)).astype(BF16)
            return carry

        lax.fori_loop(0, 4, up_tile, 0)
        ready(8)

        def down_tile(n, carry):
            cols = pl.ds(pl.multiple_of(n * 512, 512), 512)
            v = dot(wide[...], w_down[slot, :, cols])
            res[:, cols] = xs[slot, :, cols].astype(F32) + 0.5 * v
            return carry

        lax.fori_loop(0, 2, down_tile, 0)
        ready(1, 9, 10)
        act[...] = normed(res[...], vec[slot, 1]).astype(BF16)

        def proj_tile(w, store):
            def tile(n, carry):
                cols = pl.ds(pl.multiple_of(n * 512, 512), 512)
                store(cols, dot(act[...], w[slot, :, cols]).astype(BF16))
                return carry

            lax.fori_loop(0, 2, tile, 0)

        def store_key(cols, v):
            kv[slot, 0, own, cols] = v

        def store_value(cols, v):
            kv[slot, 1, own, cols] = v

        def store_query(cols, v):
            wide[:, cols] = v * jnp.asarray(0.125, BF16)

        proj_tile(w_key, store_key)
        kv_copy(slot, 0).start()
        proj_tile(w_value, store_value)
        kv_copy(slot, 1).start()
        ready(11)
        proj_tile(w_query, store_query)
        kv_arrival(slot, 0).wait_recv()
        kv_arrival(slot, 1).wait_recv()

        seen = lax.broadcasted_iota(jnp.int32, (1, LEN), 1) < length
        bias = jnp.where(seen, 0.0, -1e30).astype(F32)
        low = lax.broadcasted_iota(jnp.int32, (ROWS, 128), 1) < 64

        def head_pair(g, carry):
            cols = pl.ds(pl.multiple_of(g * 128, 128), 128)
            q = wide[:, cols]
            keys = kv[slot, 0, :, cols]
            values = kv[slot, 1, :, cols]
            mixed = []
            for part in (low, jnp.logical_not(low)):
                q_head = jnp.where(part, q, jnp.zeros_like(q))
                scores = lax.dot_general(
                    q_head, keys, (((1,), (1,)), ((), ())), preferred_element_type=F32
                )
                scores = scores + bias
                peak = jnp.max(scores, axis=-1, keepdims=True)
                weights = jnp.exp(scores - peak)
                total = jnp.sum(weights, axis=-1, keepdims=True)
                mixed.append(dot(weights.astype(BF16), values) * (1.0 / total))
            act[:, cols] = jnp.where(low, mixed[0], mixed[1]).astype(BF16)
            return carry

        lax.fori_loop(0, HEADS // 2, head_pair, 0)
        ready(12)

        def out_tile(n, carry):
            cols = pl.ds(pl.multiple_of(n * 512, 512), 512)
            res[:, cols] = res[:, cols] + dot(act[...], w_out[slot, :, cols])
            return carry

        lax.fori_loop(0, 2, out_tile, 0)
        ready(2, 13)
        wide[:, :D] = normed(res[...], vec[slot, 2]).astype(BF16)
        row = c * ROWS + lax.broadcasted_iota(jnp.int32, (ROWS, 256), 0)
        keep = (row < length).astype(F32)

        def glu_tile(n, carry):
            base = pl.multiple_of(n * 256, 256)
            value = dot(wide[:, :D], w_expand[slot, :, pl.ds(base, 256)])
            gate = dot(wide[:, :D], w_expand[slot, :, pl.ds(base + D, 256)])
            glu = (value * sigmoid(gate) * keep).astype(BF16)
            edge = jnp.where(c == 0, glu[ROWS - 16 :], glu[:16])
            rim_out[slot, :, pl.ds(base, 256)] = edge
            glu = glu.astype(F32)
            padded[2 * n, pl.ds(16, ROWS), :] = glu[:, :128]
            padded[2 * n + 1, pl.ds(16, ROWS), :] = glu[:, 128:]
            return carry

        lax.fori_loop(0, 4, glu_tile, 0)
        rim_copy(slot).start()
        ready(3, 4, 6)
        rim_copy(slot).wait_recv()
        for n in range(8):
            got = rim_in[slot, :, n * 128 : (n + 1) * 128].astype(F32)
            zero = jnp.zeros_like(got)
            padded[n, pl.ds(0, 16), :] = jnp.where(c == 0, zero, got)
            padded[n, pl.ds(16 + ROWS, 16), :] = jnp.where(c == 0, got, zero)

        def conv_tile(i, carry):
            n = i // 2
            half = lax.rem(i, 2) * 128
            cols = pl.ds(pl.multiple_of(n * 128, 128), 128)
            weights = [taps[slot, pl.ds(j, 1), cols] for j in range(TAPS)]
            sums = [None] * 16
            for o in range(1, 8 * 15 + TAPS + 1):
                v = padded[n, pl.ds(half + o, 8), :]
                for b in range(16):
                    j = o - 1 - 8 * b
                    if 0 <= j < TAPS:
                        term = v * weights[j]
                        sums[b] = term if sums[b] is None else sums[b] + term
            for b in range(16):
                depth[pl.ds(pl.multiple_of(half + 8 * b, 8), 8), cols] = sums[b]
            return carry

        lax.fori_loop(0, 16, conv_tile, 0)
        shifted = normed(depth[...], vec[slot, 3]) + vec[slot, 4]
        act[...] = (shifted * sigmoid(shifted)).astype(BF16)
        ready(14, 5)
        for h in range(2):
            rows = pl.ds(h * 128, 128)
            closing = res[rows, :] + dot(act[rows, :], w_shrink[slot])
            xs[slot + 1, rows, :] = normed(closing, vec[slot, 5]).astype(BF16)
            for j in (2 * h, 2 * h + 1):

                @pl.when((slot == 1) & (k < STAGES - 1))
                def _(j=j):
                    forward(j).start()

                @pl.when(own_piece(slot, j))
                def _(j=j):
                    scatter_local(slot, j).start()

                @pl.when(jnp.logical_not(own_piece(slot, j)))
                def _(j=j):
                    scatter(slot, j).start()

        return carry

    @pl.when(active)
    def _():
        lax.fori_loop(0, 2, run_slot, 0)
        for i in ORDER:
            push(i).wait_send()
        for slot in range(2):
            for i in range(2):
                kv_copy(slot, i).wait_send()
            rim_copy(slot).wait_send()
            for j in range(PIECES):

                @pl.when(jnp.logical_not(own_piece(slot, j)))
                def _(slot=slot, j=j):
                    scatter(slot, j).wait_send()

        @pl.when(k < STAGES - 1)
        def _():
            for j in range(PIECES):
                forward(j).wait_send()

    for v in range(UTTS):

        @pl.when(sends_frames & (t != 2 * v + 1))
        def _(v=v):
            frame_copy(v).wait_send()

    for v in range(UTTS):
        itself = (t == 2 * v + side) & (c == t // 4)
        landed = out.at[0, v]

        @pl.when(itself)
        def _(v=v, landed=landed):
            pltpu.make_async_copy(xs.at[0, piece_rows(0)], landed, out_recv.at[v]).wait()

        @pl.when(jnp.logical_not(itself))
        def _(v=v, landed=landed):
            pltpu.make_async_remote_copy(
                landed, landed, out_send.at[0, 0], out_recv.at[v], device_id=partner, device_id_type=MESH
            ).wait_recv()


def body(
    frames,
    lengths,
    ffn_gain,
    ffn_up,
    ffn_down,
    attn_gain,
    query_weight,
    key_weight,
    value_weight,
    out_weight,
    conv_gain,
    expand_weight,
    depth_weight,
    depth_gain,
    norm_shift,
    shrink_weight,
    final_gain,
):
    anywhere = pl.BlockSpec(memory_space=pl.ANY)
    dma = pltpu.SemaphoreType.DMA
    return pl.pallas_call(
        block_kernel,
        name="conformer",
        out_shape=jax.ShapeDtypeStruct((1, UTTS, PIECE, D), BF16),
        in_specs=[pl.BlockSpec(memory_space=pltpu.SMEM)] + [anywhere] * 16,
        out_specs=anywhere,
        scratch_shapes=[pltpu.VMEM((2,) + shape, BF16) for shape in SHAPES]
        + [
            pltpu.VMEM((2, 6, 1, D), F32),
            pltpu.VMEM((2, TAPS, D), F32),
            pltpu.VMEM((3, ROWS, D), BF16),
            pltpu.VMEM((ROWS, D), BF16),
            pltpu.VMEM((ROWS, FF), BF16),
            pltpu.VMEM((ROWS, D), F32),
            pltpu.VMEM((2, 2, LEN, D), BF16),
            pltpu.VMEM((2, 16, D), BF16),
            pltpu.VMEM((2, 16, D), BF16),
            pltpu.VMEM((8, ROWS + 32, 128), F32),
            pltpu.VMEM((ROWS, D), F32),
            dma((15,)),
            dma((15,)),
            dma((15,)),
            dma((PIECES,)),
            dma((PIECES,)),
            dma((2, PIECES)),
            dma((UTTS,)),
            dma((2, 2)),
            dma((2, 2)),
            dma((2,)),
            dma((2,)),
            dma((UTTS,)),
        ],
        compiler_params=pltpu.CompilerParams(
            has_side_effects=True, vmem_limit_bytes=67043328
        ),
    )(
        lengths,
        frames,
        ffn_gain,
        attn_gain,
        conv_gain,
        depth_gain,
        norm_shift,
        final_gain,
        depth_weight,
        ffn_up,
        ffn_down,
        key_weight,
        value_weight,
        query_weight,
        out_weight,
        expand_weight,
        shrink_weight,
    )


def solution(mesh):
    return jax.shard_map(
        body,
        mesh=mesh,
        in_specs=(
            P(None, "tm", None),
            P(),
            P("section", None),
            P("section", None, None),
            P("section", None, None),
            P("section", None),
            P("section", None, None),
            P("section", None, None),
            P("section", None, None),
            P("section", None, None),
            P("section", None),
            P("section", None, None),
            P("section", None, None),
            P("section", None),
            P("section", None),
            P("section", None, None),
            P("section", None),
        ),
        out_specs=P("section", None, "tm", None),
        check_vma=False,
    )
```

```python
import functools

import jax
import jax.numpy as jnp
from jax import lax
from jax.experimental import pallas as pl
from jax.experimental.pallas import tpu as pltpu
from jax.sharding import PartitionSpec as P

MESH = pl.DeviceIdType.MESH
F32 = jnp.float32
BF16 = jnp.bfloat16
EPS = 1e-05
D = 1024
FF = 2048
HEADS = 16
ROWS = 256
LEN = 512
TAPS = 31
UTTS = 4
STAGES = 8
PIECE = 64
PIECES = ROWS // PIECE
QUERY_SCALE = 0.125 * 1.4426950408889634
SHAPES = ((D, FF), (FF, D), (D, D), (D, D), (D, D), (D, D), (D, 2 * D), (D, D))


def sigmoid(v):
    return 0.5 * jnp.tanh(0.5 * v) + 0.5


def normed(v, gain):
    mean = jnp.mean(v, axis=-1, keepdims=True)
    centred = v - mean
    spread = jnp.mean(centred * centred, axis=-1, keepdims=True)
    return centred * lax.rsqrt(spread + EPS) * gain


def dot(a, b):
    return jnp.dot(a, b, preferred_element_type=F32)


def block_kernel(
    lengths,
    frames,
    ffn_gain,
    attn_gain,
    conv_gain,
    depth_gain,
    norm_shift,
    final_gain,
    depth_weight,
    h_up,
    h_down,
    h_key,
    h_value,
    h_query,
    h_out,
    h_expand,
    h_shrink,
    out,
    w_up,
    w_down,
    w_key,
    w_value,
    w_query,
    w_out,
    w_expand,
    w_shrink,
    vec,
    taps,
    xs,
    act,
    wide,
    res,
    kv,
    rim_out,
    rim_in,
    bias,
    padded,
    depth,
    local_sem,
    push_sem,
    pull_sem,
    x_send,
    x_recv,
    out_send,
    out_recv,
    kv_send,
    kv_recv,
    rim_send,
    rim_recv,
    frame_send,
):
    s = lax.axis_index("section")
    t = lax.axis_index("tm")
    k = s // 2
    c = lax.rem(s, 2)
    u = t // 2
    side = 1 - lax.rem(k, 2)
    active = lax.rem(t, 2) == side
    partner = {"section": 2 * k + 1 - c, "tm": t}
    here = {"section": s, "tm": t}
    del here

    hbm = (h_up, h_down, h_key, h_value, h_query, h_out, h_expand, h_shrink)
    vmem = (w_up, w_down, w_key, w_value, w_query, w_out, w_expand, w_shrink)
    small = (ffn_gain, attn_gain, conv_gain, depth_gain, norm_shift, final_gain)

    def sources():
        pairs = [(small[i], vec.at[c, i]) for i in range(6)]
        pairs += [(depth_weight.at[0], taps.at[c])]
        pairs += [(hbm[i].at[0], vmem[i].at[c]) for i in range(8)]
        return pairs

    def arrivals(slot):
        refs = [vec.at[slot, i] for i in range(6)] + [taps.at[slot]]
        return refs + [vmem[i].at[slot] for i in range(8)]

    def local(i):
        src, dst = sources()[i]
        return pltpu.make_async_copy(src, dst, local_sem.at[i])

    def push(i):
        src, dst = sources()[i]
        return pltpu.make_async_remote_copy(
            src, dst, push_sem.at[i], pull_sem.at[i], device_id=partner, device_id_type=MESH
        )

    def pull(i, slot):
        ref = arrivals(slot)[i]
        return pltpu.make_async_remote_copy(
            ref, ref, push_sem.at[i], pull_sem.at[i], device_id=partner, device_id_type=MESH
        )

    ORDER = (0, 7, 8, 1, 9, 10, 11, 12, 2, 6, 13, 3, 4, 14, 5)

    @pl.when(active)
    def _():
        for i in ORDER:
            local(i).start()
        for i in ORDER:
            push(i).start()

    def frame_copy(v):
        return pltpu.make_async_remote_copy(
            frames.at[v],
            xs.at[0, pl.ds(pl.multiple_of(lax.rem(t, 4) * PIECE, PIECE), PIECE)],
            frame_send.at[v],
            x_recv.at[lax.rem(t, 4)],
            device_id={"section": s, "tm": 2 * v + 1},
            device_id_type=MESH,
        )

    def frame_local(v):
        return pltpu.make_async_copy(
            frames.at[v],
            xs.at[0, pl.ds(pl.multiple_of(lax.rem(t, 4) * PIECE, PIECE), PIECE)],
            x_recv.at[lax.rem(t, 4)],
        )

    sends_frames = (k == 0) & (t // 4 == c)
    for v in range(UTTS):

        @pl.when(sends_frames & (t != 2 * v + 1))
        def _(v=v):
            frame_copy(v).start()

        @pl.when(sends_frames & (t == 2 * v + 1))
        def _(v=v):
            frame_local(v).start()

    def piece_rows(j):
        return pl.ds(j * PIECE, PIECE)

    def forward(j):
        return pltpu.make_async_remote_copy(
            xs.at[2, piece_rows(j)],
            xs.at[0, piece_rows(j)],
            x_send.at[j],
            x_recv.at[j],
            device_id={"section": lax.rem(s + 2, 16), "tm": 2 * u + 1 - side},
            device_id_type=MESH,
        )

    def scatter(slot, j):
        return pltpu.make_async_remote_copy(
            xs.at[slot + 1, piece_rows(j)],
            out.at[0, u],
            out_send.at[slot, j],
            out_recv.at[u],
            device_id={"section": 2 * k + slot, "tm": 4 * c + j},
            device_id_type=MESH,
        )

    def scatter_local(slot, j):
        return pltpu.make_async_copy(xs.at[slot + 1, piece_rows(j)], out.at[0, u], out_recv.at[u])

    def own_piece(slot, j):
        return (slot == c) & (4 * c + j == t)

    own = pl.ds(pl.multiple_of(c * ROWS, ROWS), ROWS)

    def kv_copy(slot, i):
        return pltpu.make_async_remote_copy(
            kv.at[slot, i, own],
            kv.at[slot, i, own],
            kv_send.at[slot, i],
            kv_recv.at[slot, i],
            device_id=partner,
            device_id_type=MESH,
        )

    def kv_arrival(slot, i):
        other = pl.ds(pl.multiple_of((1 - c) * ROWS, ROWS), ROWS)
        return pltpu.make_async_remote_copy(
            kv.at[slot, i, other],
            kv.at[slot, i, other],
            kv_send.at[slot, i],
            kv_recv.at[slot, i],
            device_id=partner,
            device_id_type=MESH,
        )

    def rim_copy(slot):
        return pltpu.make_async_remote_copy(
            rim_out.at[slot],
            rim_in.at[slot],
            rim_send.at[slot],
            rim_recv.at[slot],
            device_id=partner,
            device_id_type=MESH,
        )

    def run_slot(slot, carry):
        mine = slot == c

        def ready(*ids):
            for i in ids:

                @pl.when(mine)
                def _(i=i):
                    local(i).wait()

                @pl.when(jnp.logical_not(mine))
                def _(i=i):
                    pull(i, slot).wait_recv()

        length = lengths[u]

        @pl.when(slot == 0)
        def _():
            for j in range(PIECES):
                itself = (k == 0) & (4 * c + j == t)

                @pl.when(itself)
                def _():
                    for v in range(UTTS):

                        @pl.when(t == 2 * v + 1)
                        def _(v=v):
                            frame_local(v).wait()

                @pl.when(jnp.logical_not(itself))
                def _(j=j):
                    forward(j).wait_recv()

        ready(0, 7)
        act[...] = normed(xs[slot].astype(F32), vec[slot, 0]).astype(BF16)

        def up_tile(n):
            cols = pl.ds(n * 512, 512)
            v = dot(act[...], w_up[slot, :, cols])
            wide[:, cols] = (v * sigmoid(v)).astype(BF16)

        for n in range(4):
            up_tile(n)
        ready(8)

        def down_tile(n):
            cols = pl.ds(n * 512, 512)
            v = dot(wide[...], w_down[slot, :, cols])
            res[:, cols] = xs[slot, :, cols].astype(F32) + 0.5 * v

        for n in range(2):
            down_tile(n)
        ready(1, 9, 10)
        act[...] = normed(res[...], vec[slot, 1]).astype(BF16)

        def proj_tile(w, store):
            def tile(n):
                cols = pl.ds(n * 512, 512)
                store(cols, dot(act[...], w[slot, :, cols]))

            for n in range(2):
                tile(n)

        def store_key(cols, v):
            kv[slot, 0, own, cols] = v.astype(BF16)

        def store_value(cols, v):
            kv[slot, 1, own, cols] = v.astype(BF16)

        def store_query(cols, v):
            wide[:, cols] = (v * QUERY_SCALE).astype(BF16)

        proj_tile(w_key, store_key)
        kv_copy(slot, 0).start()
        proj_tile(w_value, store_value)
        kv_copy(slot, 1).start()
        ready(11)
        proj_tile(w_query, store_query)
        kv_arrival(slot, 0).wait_recv()
        kv_arrival(slot, 1).wait_recv()

        low = lax.broadcasted_iota(jnp.int32, (ROWS, 128), 1) < 64
        one = jnp.where(lax.broadcasted_iota(jnp.int32, (ROWS, 128), 1) == 0, 1.0, 0.0).astype(BF16)
        ones = jnp.ones((LEN, 128), BF16)

        def pair_scores(g):
            cols = pl.ds(g * 128, 128)
            q = wide[:, cols]
            none = jnp.zeros_like(q)
            stacked = jnp.concatenate(
                [
                    jnp.concatenate([jnp.where(low, q, none), one], axis=1),
                    jnp.concatenate([jnp.where(low, none, q), one], axis=1),
                ],
                axis=0,
            )
            keys = jnp.concatenate([kv[slot, 0, :, cols], bias[...]], axis=1)
            return lax.dot_general(
                stacked, keys, (((1,), (1,)), ((), ())), preferred_element_type=F32
            )

        def pair_context(g, scores):
            cols = pl.ds(g * 128, 128)
            peak = jnp.max(scores, axis=-1, keepdims=True)
            weights = jnp.exp2(scores - peak).astype(BF16)
            values = jnp.concatenate([kv[slot, 1, :, cols], ones], axis=1)
            mixed = dot(weights, values)
            total = jnp.where(low, mixed[:ROWS, 128:], mixed[ROWS:, 128:])
            mixed = jnp.where(low, mixed[:ROWS, :128], mixed[ROWS:, :128])
            act[:, cols] = (mixed / total).astype(BF16)

        scores = pair_scores(0)
        for g in range(HEADS // 2):
            later = pair_scores(g + 1) if g + 1 < HEADS // 2 else None
            pair_context(g, scores)
            scores = later
        ready(12)

        def out_tile(n):
            cols = pl.ds(n * 512, 512)
            res[:, cols] = res[:, cols] + dot(act[...], w_out[slot, :, cols])

        for n in range(2):
            out_tile(n)
        ready(2, 13, 6)
        wide[:, :D] = normed(res[...], vec[slot, 2]).astype(BF16)
        row = c * ROWS + lax.broadcasted_iota(jnp.int32, (ROWS, 256), 0)
        keep = (row < length).astype(F32)

        def glu_tile(n):
            value = dot(wide[:, :D], w_expand[slot, :, pl.ds(n * 256, 256)])
            gate = dot(wide[:, :D], w_expand[slot, :, pl.ds(n * 256 + D, 256)])
            glu = (value * sigmoid(gate) * keep).astype(BF16)
            rim_out[slot, :, pl.ds(n * 256, 256)] = jnp.where(c == 0, glu[ROWS - 16 :], glu[:16])
            glu = glu.astype(F32)
            padded[2 * n, pl.ds(16, ROWS), :] = glu[:, :128]
            padded[2 * n + 1, pl.ds(16, ROWS), :] = glu[:, 128:]

        def conv_rows(n, base, blocks):
            cols = pl.ds(n * 128, 128)
            weights = [taps[slot, pl.ds(j, 1), cols] for j in range(TAPS)]
            sums = [None] * blocks
            for o in range(1, 8 * (blocks - 1) + TAPS + 1):
                v = padded[n, pl.ds(base + o, 8), :]
                for b in range(blocks):
                    j = o - 1 - 8 * b
                    if 0 <= j < TAPS:
                        term = v * weights[j]
                        sums[b] = term if sums[b] is None else sums[b] + term
            for b in range(blocks):
                depth[pl.ds(base + 8 * b, 8), cols] = sums[b]

        for n in range(5):
            if n < 4:
                glu_tile(n)
            if n > 0:
                for i in (2 * n - 2, 2 * n - 1):
                    conv_rows(i, 0, 16)
                    conv_rows(i, 128, 16)
        rim_copy(slot).start()
        ready(3, 4)
        rim_copy(slot).wait_recv()
        inner_rim = pl.ds(pl.multiple_of((1 - c) * (ROWS + 16), 16), 16)
        edge = pl.multiple_of((1 - c) * (ROWS - 16), 16)
        for n in range(8):
            padded[n, inner_rim, :] = rim_in[slot, :, n * 128 : (n + 1) * 128].astype(F32)
            conv_rows(n, edge, 2)
        shifted = normed(depth[...], vec[slot, 3]) + vec[slot, 4]
        act[...] = (shifted * sigmoid(shifted)).astype(BF16)
        ready(14, 5)
        for h in range(2):
            rows = pl.ds(h * 128, 128)
            closing = res[rows, :] + dot(act[rows, :], w_shrink[slot])
            xs[slot + 1, rows, :] = normed(closing, vec[slot, 5]).astype(BF16)
            for j in (2 * h, 2 * h + 1):

                @pl.when((slot == 1) & (k < STAGES - 1))
                def _(j=j):
                    forward(j).start()

                @pl.when(own_piece(slot, j))
                def _(j=j):
                    scatter_local(slot, j).start()

                @pl.when(jnp.logical_not(own_piece(slot, j)))
                def _(j=j):
                    scatter(slot, j).start()

        return carry

    @pl.when(active)
    def _():
        seen = lax.broadcasted_iota(jnp.int32, (LEN, 128), 0) < lengths[u]
        bias[...] = jnp.where(seen, 0.0, -1e30).astype(BF16)
        for n in range(8):
            padded[n, pl.ds(0, 16), :] = jnp.zeros((16, 128), F32)
            padded[n, pl.ds(16 + ROWS, 16), :] = jnp.zeros((16, 128), F32)
        lax.fori_loop(0, 2, run_slot, 0)
        for i in ORDER:
            push(i).wait_send()
        for slot in range(2):
            for i in range(2):
                kv_copy(slot, i).wait_send()
            rim_copy(slot).wait_send()
            for j in range(PIECES):

                @pl.when(jnp.logical_not(own_piece(slot, j)))
                def _(slot=slot, j=j):
                    scatter(slot, j).wait_send()

        @pl.when(k < STAGES - 1)
        def _():
            for j in range(PIECES):
                forward(j).wait_send()

    for v in range(UTTS):

        @pl.when(sends_frames & (t != 2 * v + 1))
        def _(v=v):
            frame_copy(v).wait_send()

    for v in range(UTTS):
        itself = (t == 2 * v + side) & (c == t // 4)
        landed = out.at[0, v]

        @pl.when(itself)
        def _(v=v, landed=landed):
            pltpu.make_async_copy(xs.at[0, piece_rows(0)], landed, out_recv.at[v]).wait()

        @pl.when(jnp.logical_not(itself))
        def _(v=v, landed=landed):
            pltpu.make_async_remote_copy(
                landed, landed, out_send.at[0, 0], out_recv.at[v], device_id=partner, device_id_type=MESH
            ).wait_recv()


def body(
    frames,
    lengths,
    ffn_gain,
    ffn_up,
    ffn_down,
    attn_gain,
    query_weight,
    key_weight,
    value_weight,
    out_weight,
    conv_gain,
    expand_weight,
    depth_weight,
    depth_gain,
    norm_shift,
    shrink_weight,
    final_gain,
):
    anywhere = pl.BlockSpec(memory_space=pl.ANY)
    dma = pltpu.SemaphoreType.DMA
    return pl.pallas_call(
        block_kernel,
        name="conformer",
        out_shape=jax.ShapeDtypeStruct((1, UTTS, PIECE, D), BF16),
        in_specs=[pl.BlockSpec(memory_space=pltpu.SMEM)] + [anywhere] * 16,
        out_specs=anywhere,
        scratch_shapes=[pltpu.VMEM((2,) + shape, BF16) for shape in SHAPES]
        + [
            pltpu.VMEM((2, 6, 1, D), F32),
            pltpu.VMEM((2, TAPS, D), F32),
            pltpu.VMEM((3, ROWS, D), BF16),
            pltpu.VMEM((ROWS, D), BF16),
            pltpu.VMEM((ROWS, FF), BF16),
            pltpu.VMEM((ROWS, D), F32),
            pltpu.VMEM((2, 2, LEN, D), BF16),
            pltpu.VMEM((2, 16, D), BF16),
            pltpu.VMEM((2, 16, D), BF16),
            pltpu.VMEM((LEN, 128), BF16),
            pltpu.VMEM((8, ROWS + 32, 128), F32),
            pltpu.VMEM((ROWS, D), F32),
            dma((15,)),
            dma((15,)),
            dma((15,)),
            dma((PIECES,)),
            dma((PIECES,)),
            dma((2, PIECES)),
            dma((UTTS,)),
            dma((2, 2)),
            dma((2, 2)),
            dma((2,)),
            dma((2,)),
            dma((UTTS,)),
        ],
        compiler_params=pltpu.CompilerParams(
            has_side_effects=True, vmem_limit_bytes=67043328
        ),
    )(
        lengths,
        frames,
        ffn_gain,
        attn_gain,
        conv_gain,
        depth_gain,
        norm_shift,
        final_gain,
        depth_weight,
        ffn_up,
        ffn_down,
        key_weight,
        value_weight,
        query_weight,
        out_weight,
        expand_weight,
        shrink_weight,
    )


def solution(mesh):
    return jax.shard_map(
        body,
        mesh=mesh,
        in_specs=(
            P(None, "tm", None),
            P(),
            P("section", None),
            P("section", None, None),
            P("section", None, None),
            P("section", None),
            P("section", None, None),
            P("section", None, None),
            P("section", None, None),
            P("section", None, None),
            P("section", None),
            P("section", None, None),
            P("section", None, None),
            P("section", None),
            P("section", None),
            P("section", None, None),
            P("section", None),
        ),
        out_specs=P("section", None, "tm", None),
        check_vma=False,
    )
```

```python
import functools

import jax
import jax.numpy as jnp
from jax import lax
from jax.experimental import pallas as pl
from jax.experimental.pallas import tpu as pltpu
from jax.sharding import PartitionSpec as P

MESH = pl.DeviceIdType.MESH
F32 = jnp.float32
BF16 = jnp.bfloat16
EPS = 1e-05
D = 1024
FF = 2048
HEADS = 16
ROWS = 256
LEN = 512
TAPS = 31
UTTS = 4
STAGES = 8
PIECE = 64
PIECES = ROWS // PIECE
HALF = ROWS // 2
QUERY_SCALE = 0.125 * 1.4426950408889634
SHAPES = ((D, FF), (FF, D), (D, D), (D, D), (D, D), (D, D), (D, 2 * D), (D, D))


def sigmoid(v):
    return 0.5 * jnp.tanh(0.5 * v) + 0.5


def normed(v, gain):
    mean = jnp.mean(v, axis=-1, keepdims=True)
    centred = v - mean
    spread = jnp.mean(centred * centred, axis=-1, keepdims=True)
    return centred * lax.rsqrt(spread + EPS) * gain


def dot(a, b):
    return jnp.dot(a, b, preferred_element_type=F32)


def block_kernel(
    lengths,
    frames,
    ffn_gain,
    attn_gain,
    conv_gain,
    depth_gain,
    norm_shift,
    final_gain,
    depth_weight,
    h_up,
    h_down,
    h_key,
    h_value,
    h_query,
    h_out,
    h_expand,
    h_shrink,
    out,
    w_up,
    w_down,
    w_key,
    w_value,
    w_query,
    w_out,
    w_expand,
    w_shrink,
    vec,
    taps,
    xs,
    act,
    wide,
    res,
    kv,
    rim_out,
    rim_in,
    bias,
    padded,
    depth,
    local_sem,
    push_sem,
    pull_sem,
    x_send,
    x_recv,
    out_send,
    out_recv,
    kv_send,
    kv_recv,
    rim_send,
    rim_recv,
    frame_send,
):
    s = lax.axis_index("section")
    t = lax.axis_index("tm")
    k = s // 2
    c = lax.rem(s, 2)
    u = t // 2
    side = 1 - lax.rem(k, 2)
    active = lax.rem(t, 2) == side
    partner = {"section": 2 * k + 1 - c, "tm": t}
    here = {"section": s, "tm": t}
    del here

    hbm = (h_up, h_down, h_key, h_value, h_query, h_out, h_expand, h_shrink)
    vmem = (w_up, w_down, w_key, w_value, w_query, w_out, w_expand, w_shrink)
    small = (ffn_gain, attn_gain, conv_gain, depth_gain, norm_shift, final_gain)

    def sources():
        pairs = [(small[i], vec.at[c, i]) for i in range(6)]
        pairs += [(depth_weight.at[0], taps.at[c])]
        pairs += [(hbm[i].at[0], vmem[i].at[c]) for i in range(8)]
        return pairs

    def arrivals(slot):
        refs = [vec.at[slot, i] for i in range(6)] + [taps.at[slot]]
        return refs + [vmem[i].at[slot] for i in range(8)]

    def local(i):
        src, dst = sources()[i]
        return pltpu.make_async_copy(src, dst, local_sem.at[i])

    def push(i):
        src, dst = sources()[i]
        return pltpu.make_async_remote_copy(
            src, dst, push_sem.at[i], pull_sem.at[i], device_id=partner, device_id_type=MESH
        )

    def pull(i, slot):
        ref = arrivals(slot)[i]
        return pltpu.make_async_remote_copy(
            ref, ref, push_sem.at[i], pull_sem.at[i], device_id=partner, device_id_type=MESH
        )

    ORDER = (0, 7, 8, 1, 9, 10, 11, 12, 2, 6, 13, 3, 4, 14, 5)

    @pl.when(active)
    def _():
        for i in ORDER:
            local(i).start()
        for i in ORDER:
            push(i).start()

    def frame_copy(v):
        return pltpu.make_async_remote_copy(
            frames.at[v],
            xs.at[0, pl.ds(pl.multiple_of(lax.rem(t, 4) * PIECE, PIECE), PIECE)],
            frame_send.at[v],
            x_recv.at[lax.rem(t, 4)],
            device_id={"section": s, "tm": 2 * v + 1},
            device_id_type=MESH,
        )

    def frame_local(v):
        return pltpu.make_async_copy(
            frames.at[v],
            xs.at[0, pl.ds(pl.multiple_of(lax.rem(t, 4) * PIECE, PIECE), PIECE)],
            x_recv.at[lax.rem(t, 4)],
        )

    sends_frames = (k == 0) & (t // 4 == c)
    for v in range(UTTS):

        @pl.when(sends_frames & (t != 2 * v + 1))
        def _(v=v):
            frame_copy(v).start()

        @pl.when(sends_frames & (t == 2 * v + 1))
        def _(v=v):
            frame_local(v).start()

    def piece_rows(j):
        return pl.ds(j * PIECE, PIECE)

    def forward(j):
        return pltpu.make_async_remote_copy(
            xs.at[2, piece_rows(j)],
            xs.at[0, piece_rows(j)],
            x_send.at[j],
            x_recv.at[j],
            device_id={"section": lax.rem(s + 2, 16), "tm": 2 * u + 1 - side},
            device_id_type=MESH,
        )

    def scatter(slot, j):
        return pltpu.make_async_remote_copy(
            xs.at[slot + 1, piece_rows(j)],
            out.at[0, u],
            out_send.at[slot, j],
            out_recv.at[u],
            device_id={"section": 2 * k + slot, "tm": 4 * c + j},
            device_id_type=MESH,
        )

    def scatter_local(slot, j):
        return pltpu.make_async_copy(xs.at[slot + 1, piece_rows(j)], out.at[0, u], out_recv.at[u])

    def own_piece(slot, j):
        return (slot == c) & (4 * c + j == t)

    own = pl.ds(pl.multiple_of(c * ROWS, ROWS), ROWS)

    def kv_part(slot, i, rows):
        ref = kv.at[slot, i // 2, rows, pl.ds((i % 2) * 512, 512)]
        return pltpu.make_async_remote_copy(
            ref, ref, kv_send.at[slot, i], kv_recv.at[slot, i], device_id=partner, device_id_type=MESH
        )

    def kv_copy(slot, i):
        return kv_part(slot, i, own)

    def kv_arrival(slot, i):
        return kv_part(slot, i, pl.ds(pl.multiple_of((1 - c) * ROWS, ROWS), ROWS))

    def rim_copy(slot):
        return pltpu.make_async_remote_copy(
            rim_out.at[slot],
            rim_in.at[slot],
            rim_send.at[slot],
            rim_recv.at[slot],
            device_id=partner,
            device_id_type=MESH,
        )

    def run_slot(slot, carry):
        mine = slot == c

        def ready(*ids):
            for i in ids:

                @pl.when(mine)
                def _(i=i):
                    local(i).wait()

                @pl.when(jnp.logical_not(mine))
                def _(i=i):
                    pull(i, slot).wait_recv()

        length = lengths[u]

        def input_ready(j):
            itself = (k == 0) & (4 * c + j == t)

            @pl.when(itself)
            def _():
                for v in range(UTTS):

                    @pl.when(t == 2 * v + 1)
                    def _(v=v):
                        frame_local(v).wait()

            @pl.when(jnp.logical_not(itself))
            def _():
                forward(j).wait_recv()

        ready(0, 7, 8)
        for h in range(2):
            rows = pl.ds(h * HALF, HALF)

            @pl.when(slot == 0)
            def _(h=h):
                for j in range(h * PIECES // 2, (h + 1) * PIECES // 2):
                    input_ready(j)

            first = normed(xs[slot, rows].astype(F32), vec[slot, 0]).astype(BF16)
            act[rows] = first
            for n in range(4):
                cols = pl.ds(n * 512, 512)
                v = dot(act[rows], w_up[slot, :, cols])
                wide[rows, cols] = (v * sigmoid(v)).astype(BF16)
            for n in range(2):
                cols = pl.ds(n * 512, 512)
                v = dot(wide[rows], w_down[slot, :, cols])
                res[rows, cols] = xs[slot, rows, cols].astype(F32) + 0.5 * v
        ready(1, 9, 10)
        act[...] = normed(res[...], vec[slot, 1]).astype(BF16)
        for i in range(4):
            cols = pl.ds((i // 2) * 512, 512)
            w = (w_key, w_value)[i % 2]
            kv[slot, i % 2, own, cols] = dot(act[...], w[slot, :, cols]).astype(BF16)
            kv_copy(slot, 2 * (i % 2) + i // 2).start()
        ready(11)
        for n in range(2):
            cols = pl.ds(n * 512, 512)
            wide[:, cols] = (dot(act[...], w_query[slot, :, cols]) * QUERY_SCALE).astype(BF16)
        kv_arrival(slot, 0).wait_recv()
        kv_arrival(slot, 2).wait_recv()

        low = lax.broadcasted_iota(jnp.int32, (ROWS, 128), 1) < 64
        one = jnp.where(lax.broadcasted_iota(jnp.int32, (ROWS, 128), 1) == 0, 1.0, 0.0).astype(BF16)
        ones = jnp.ones((LEN, 128), BF16)

        def pair_scores(g):
            cols = pl.ds(g * 128, 128)
            q = wide[:, cols]
            none = jnp.zeros_like(q)
            stacked = jnp.concatenate(
                [
                    jnp.concatenate([jnp.where(low, q, none), one], axis=1),
                    jnp.concatenate([jnp.where(low, none, q), one], axis=1),
                ],
                axis=0,
            )
            keys = jnp.concatenate([kv[slot, 0, :, cols], bias[...]], axis=1)
            return lax.dot_general(
                stacked, keys, (((1,), (1,)), ((), ())), preferred_element_type=F32
            )

        def pair_context(g, scores):
            cols = pl.ds(g * 128, 128)
            peak = jnp.max(scores, axis=-1, keepdims=True)
            weights = jnp.exp2(scores - peak).astype(BF16)
            values = jnp.concatenate([kv[slot, 1, :, cols], ones], axis=1)
            mixed = dot(weights, values)
            total = jnp.where(low, mixed[:ROWS, 128:], mixed[ROWS:, 128:])
            mixed = jnp.where(low, mixed[:ROWS, :128], mixed[ROWS:, :128])
            act[:, cols] = (mixed / total).astype(BF16)

        scores = pair_scores(0)
        for g in range(HEADS // 2):
            if g == 3:
                kv_arrival(slot, 1).wait_recv()
                kv_arrival(slot, 3).wait_recv()
            later = pair_scores(g + 1) if g + 1 < HEADS // 2 else None
            pair_context(g, scores)
            scores = later
        ready(12)

        def out_tile(n):
            cols = pl.ds(n * 512, 512)
            res[:, cols] = res[:, cols] + dot(act[...], w_out[slot, :, cols])

        for n in range(2):
            out_tile(n)
        ready(2, 13, 6)
        wide[:, :D] = normed(res[...], vec[slot, 2]).astype(BF16)
        row = c * ROWS + lax.broadcasted_iota(jnp.int32, (ROWS, 256), 0)
        keep = (row < length).astype(F32)

        def glu_tile(n):
            value = dot(wide[:, :D], w_expand[slot, :, pl.ds(n * 256, 256)])
            gate = dot(wide[:, :D], w_expand[slot, :, pl.ds(n * 256 + D, 256)])
            glu = (value * sigmoid(gate) * keep).astype(BF16)
            rim_out[slot, :, pl.ds(n * 256, 256)] = jnp.where(c == 0, glu[ROWS - 16 :], glu[:16])
            glu = glu.astype(F32)
            padded[2 * n, pl.ds(16, ROWS), :] = glu[:, :128]
            padded[2 * n + 1, pl.ds(16, ROWS), :] = glu[:, 128:]

        def conv_rows(n, base, blocks):
            cols = pl.ds(n * 128, 128)
            weights = [taps[slot, pl.ds(j, 1), cols] for j in range(TAPS)]
            sums = [None] * blocks
            for o in range(1, 8 * (blocks - 1) + TAPS + 1):
                v = padded[n, pl.ds(base + o, 8), :]
                for b in range(blocks):
                    j = o - 1 - 8 * b
                    if 0 <= j < TAPS:
                        term = v * weights[j]
                        sums[b] = term if sums[b] is None else sums[b] + term
            for b in range(blocks):
                depth[pl.ds(base + 8 * b, 8), cols] = sums[b]

        for n in range(5):
            if n < 4:
                glu_tile(n)
            if n == 3:
                rim_copy(slot).start()
            if n > 0:
                for i in (2 * n - 2, 2 * n - 1):
                    conv_rows(i, 0, 16)
                    conv_rows(i, 128, 16)
        ready(3, 4)
        rim_copy(slot).wait_recv()
        inner_rim = pl.ds(pl.multiple_of((1 - c) * (ROWS + 16), 16), 16)
        edge = pl.multiple_of((1 - c) * (ROWS - 16), 16)
        for n in range(8):
            padded[n, inner_rim, :] = rim_in[slot, :, n * 128 : (n + 1) * 128].astype(F32)
            conv_rows(n, edge, 2)
        ready(14, 5)
        for h in range(2):
            rows = pl.ds(h * HALF, HALF)
            shifted = normed(depth[rows], vec[slot, 3]) + vec[slot, 4]
            act[rows] = (shifted * sigmoid(shifted)).astype(BF16)
            closing = res[rows] + dot(act[rows], w_shrink[slot])
            xs[slot + 1, rows] = normed(closing, vec[slot, 5]).astype(BF16)
            for j in (2 * h, 2 * h + 1):

                @pl.when((slot == 1) & (k < STAGES - 1))
                def _(j=j):
                    forward(j).start()

                @pl.when(own_piece(slot, j))
                def _(j=j):
                    scatter_local(slot, j).start()

                @pl.when(jnp.logical_not(own_piece(slot, j)))
                def _(j=j):
                    scatter(slot, j).start()

        return carry

    @pl.when(active)
    def _():
        seen = lax.broadcasted_iota(jnp.int32, (LEN, 128), 0) < lengths[u]
        bias[...] = jnp.where(seen, 0.0, -1e30).astype(BF16)
        for n in range(8):
            padded[n, pl.ds(0, 16), :] = jnp.zeros((16, 128), F32)
            padded[n, pl.ds(16 + ROWS, 16), :] = jnp.zeros((16, 128), F32)
        lax.fori_loop(0, 2, run_slot, 0)
        for i in ORDER:
            push(i).wait_send()
        for slot in range(2):
            for i in range(4):
                kv_copy(slot, i).wait_send()
            rim_copy(slot).wait_send()
            for j in range(PIECES):

                @pl.when(jnp.logical_not(own_piece(slot, j)))
                def _(slot=slot, j=j):
                    scatter(slot, j).wait_send()

        @pl.when(k < STAGES - 1)
        def _():
            for j in range(PIECES):
                forward(j).wait_send()

    for v in range(UTTS):

        @pl.when(sends_frames & (t != 2 * v + 1))
        def _(v=v):
            frame_copy(v).wait_send()

    for v in range(UTTS):
        itself = (t == 2 * v + side) & (c == t // 4)
        landed = out.at[0, v]

        @pl.when(itself)
        def _(v=v, landed=landed):
            pltpu.make_async_copy(xs.at[0, piece_rows(0)], landed, out_recv.at[v]).wait()

        @pl.when(jnp.logical_not(itself))
        def _(v=v, landed=landed):
            pltpu.make_async_remote_copy(
                landed, landed, out_send.at[0, 0], out_recv.at[v], device_id=partner, device_id_type=MESH
            ).wait_recv()


def body(
    frames,
    lengths,
    ffn_gain,
    ffn_up,
    ffn_down,
    attn_gain,
    query_weight,
    key_weight,
    value_weight,
    out_weight,
    conv_gain,
    expand_weight,
    depth_weight,
    depth_gain,
    norm_shift,
    shrink_weight,
    final_gain,
):
    anywhere = pl.BlockSpec(memory_space=pl.ANY)
    dma = pltpu.SemaphoreType.DMA
    return pl.pallas_call(
        block_kernel,
        name="conformer",
        out_shape=jax.ShapeDtypeStruct((1, UTTS, PIECE, D), BF16),
        in_specs=[pl.BlockSpec(memory_space=pltpu.SMEM)] + [anywhere] * 16,
        out_specs=anywhere,
        scratch_shapes=[pltpu.VMEM((2,) + shape, BF16) for shape in SHAPES]
        + [
            pltpu.VMEM((2, 6, 1, D), F32),
            pltpu.VMEM((2, TAPS, D), F32),
            pltpu.VMEM((3, ROWS, D), BF16),
            pltpu.VMEM((ROWS, D), BF16),
            pltpu.VMEM((ROWS, FF), BF16),
            pltpu.VMEM((ROWS, D), F32),
            pltpu.VMEM((2, 2, LEN, D), BF16),
            pltpu.VMEM((2, 16, D), BF16),
            pltpu.VMEM((2, 16, D), BF16),
            pltpu.VMEM((LEN, 128), BF16),
            pltpu.VMEM((8, ROWS + 32, 128), F32),
            pltpu.VMEM((ROWS, D), F32),
            dma((15,)),
            dma((15,)),
            dma((15,)),
            dma((PIECES,)),
            dma((PIECES,)),
            dma((2, PIECES)),
            dma((UTTS,)),
            dma((2, 4)),
            dma((2, 4)),
            dma((2,)),
            dma((2,)),
            dma((UTTS,)),
        ],
        compiler_params=pltpu.CompilerParams(
            has_side_effects=True, vmem_limit_bytes=67043328
        ),
    )(
        lengths,
        frames,
        ffn_gain,
        attn_gain,
        conv_gain,
        depth_gain,
        norm_shift,
        final_gain,
        depth_weight,
        ffn_up,
        ffn_down,
        key_weight,
        value_weight,
        query_weight,
        out_weight,
        expand_weight,
        shrink_weight,
    )


def solution(mesh):
    return jax.shard_map(
        body,
        mesh=mesh,
        in_specs=(
            P(None, "tm", None),
            P(),
            P("section", None),
            P("section", None, None),
            P("section", None, None),
            P("section", None),
            P("section", None, None),
            P("section", None, None),
            P("section", None, None),
            P("section", None, None),
            P("section", None),
            P("section", None, None),
            P("section", None, None),
            P("section", None),
            P("section", None),
            P("section", None, None),
            P("section", None),
        ),
        out_specs=P("section", None, "tm", None),
        check_vma=False,
    )
```

```python
import functools

import jax
import jax.numpy as jnp
from jax import lax
from jax.experimental import pallas as pl
from jax.experimental.pallas import tpu as pltpu
from jax.sharding import PartitionSpec as P

MESH = pl.DeviceIdType.MESH
F32 = jnp.float32
BF16 = jnp.bfloat16
EPS = 1e-05
D = 1024
FF = 2048
HEADS = 16
ROWS = 256
LEN = 512
TAPS = 31
UTTS = 4
STAGES = 8
PIECE = 64
PIECES = ROWS // PIECE
HALF = ROWS // 2
QUERY_SCALE = 0.125 * 1.4426950408889634
SHAPES = ((D, FF), (FF, D), (D, D), (D, D), (D, D), (D, D), (D, 2 * D), (D, D))


def sigmoid(v):
    return 0.5 * jnp.tanh(0.5 * v) + 0.5


def normed(v, gain):
    mean = jnp.mean(v, axis=-1, keepdims=True)
    centred = v - mean
    spread = jnp.mean(centred * centred, axis=-1, keepdims=True)
    return centred * lax.rsqrt(spread + EPS) * gain


def dot(a, b):
    return jnp.dot(a, b, preferred_element_type=F32)


def block_kernel(
    lengths,
    frames,
    ffn_gain,
    attn_gain,
    conv_gain,
    depth_gain,
    norm_shift,
    final_gain,
    depth_weight,
    h_up,
    h_down,
    h_key,
    h_value,
    h_query,
    h_out,
    h_expand,
    h_shrink,
    out,
    w_up,
    w_down,
    w_key,
    w_value,
    w_query,
    w_out,
    w_expand,
    w_shrink,
    vec,
    taps,
    xs,
    act,
    wide,
    sums,
    kv,
    rim_out,
    rim_in,
    bias,
    padded,
    via_x,
    via_z,
    local_sem,
    push_sem,
    pull_sem,
    x_send,
    x_recv,
    out_send,
    out_recv,
    kv_send,
    kv_recv,
    rim_send,
    rim_recv,
    frame_send,
    via_send,
    via_recv,
    hand_send,
    hand_recv,
):
    res, depth = sums.at[0], sums.at[1]
    s = lax.axis_index("section")
    t = lax.axis_index("tm")
    k = s // 2
    c = lax.rem(s, 2)
    u = t // 2
    side = 1 - lax.rem(k, 2)
    active = lax.rem(t, 2) == side
    partner = {"section": 2 * k + 1 - c, "tm": t}
    here = {"section": s, "tm": t}
    del here

    hbm = (h_up, h_down, h_key, h_value, h_query, h_out, h_expand, h_shrink)
    vmem = (w_up, w_down, w_key, w_value, w_query, w_out, w_expand, w_shrink)
    small = (ffn_gain, attn_gain, conv_gain, depth_gain, norm_shift, final_gain)

    def sources():
        pairs = [(small[i], vec.at[c, i]) for i in range(6)]
        pairs += [(depth_weight.at[0], taps.at[c])]
        pairs += [(hbm[i].at[0], vmem[i].at[c]) for i in range(8)]
        return pairs

    def arrivals(slot):
        refs = [vec.at[slot, i] for i in range(6)] + [taps.at[slot]]
        return refs + [vmem[i].at[slot] for i in range(8)]

    def local(i):
        src, dst = sources()[i]
        return pltpu.make_async_copy(src, dst, local_sem.at[i])

    def push(i):
        src, dst = sources()[i]
        return pltpu.make_async_remote_copy(
            src, dst, push_sem.at[i], pull_sem.at[i], device_id=partner, device_id_type=MESH
        )

    def pull(i, slot):
        ref = arrivals(slot)[i]
        return pltpu.make_async_remote_copy(
            ref, ref, push_sem.at[i], pull_sem.at[i], device_id=partner, device_id_type=MESH
        )

    lead = (k == 0) & (c == 0)

    def pushed(i):
        return jnp.logical_not(lead) if i in (0, 7, 8) else k >= 0

    ORDER = (0, 7, 8, 1, 9, 10, 11, 12, 2, 6, 13, 3, 4, 14, 5)

    @pl.when(active)
    def _():
        for i in ORDER:
            local(i).start()
        for i in ORDER:

            @pl.when(pushed(i))
            def _(i=i):
                push(i).start()


    frame_rows = xs.at[t // 4, pl.ds(pl.multiple_of(lax.rem(t, 4) * PIECE, PIECE), PIECE)]

    def frame_copy(v):
        return pltpu.make_async_remote_copy(
            frames.at[v],
            frame_rows,
            frame_send.at[v],
            x_recv.at[t],
            device_id={"section": 0, "tm": 2 * v + 1},
            device_id_type=MESH,
        )

    def frame_local(v):
        return pltpu.make_async_copy(frames.at[v], frame_rows, x_recv.at[t])

    sends_frames = (k == 0) & (t // 4 == c)
    for v in range(UTTS):
        to_itself = (c == 0) & (t == 2 * v + 1)

        @pl.when(sends_frames & jnp.logical_not(to_itself))
        def _(v=v):
            frame_copy(v).start()

        @pl.when(sends_frames & to_itself)
        def _(v=v):
            frame_local(v).start()

    def piece_rows(j):
        return pl.ds(j * PIECE, PIECE)

    def forward(j):
        return pltpu.make_async_remote_copy(
            xs.at[2, piece_rows(j)],
            xs.at[0, piece_rows(j)],
            x_send.at[j],
            x_recv.at[j],
            device_id={"section": lax.rem(s + 2, 16), "tm": 2 * u + 1 - side},
            device_id_type=MESH,
        )

    def relayed(src, dst, send, recv, section, tm):
        return pltpu.make_async_remote_copy(
            src, dst, send, recv, device_id={"section": lax.rem(section + 16, 16), "tm": tm}, device_id_type=MESH
        )

    even = lax.rem(k, 2) == 0
    first_piece = xs.at[0, pl.ds(0, PIECE)]
    last_first = xs.at[2, pl.ds(0, PIECE)]

    def leave_x():
        return relayed(last_first, via_x, x_send.at[0], via_recv.at[0], s, 2 * u)

    def leave_z():
        return relayed(last_first, via_z, x_send.at[0], via_recv.at[1], s + 4, 2 * u + 1)

    def pass_x():
        return relayed(via_x, via_x, via_send.at[0], via_recv.at[0], s + 2, 2 * u + 1)

    def land_x():
        return relayed(via_x, first_piece, via_send.at[0], x_recv.at[0], s, 2 * u)

    def land_z():
        return relayed(via_z, first_piece, via_send.at[1], x_recv.at[0], s - 2, 2 * u + 1)

    idle = jnp.logical_not(active)

    @pl.when(idle & even)
    def _():
        pass_x().wait_recv()
        pass_x().start()
        pass_x().wait_send()

    @pl.when(idle & jnp.logical_not(even))
    def _():
        @pl.when(k >= 3)
        def _():
            leave_z().wait_recv()
            land_z().start()
            land_z().wait_send()

        pass_x().wait_recv()
        land_x().start()
        land_x().wait_send()

    def scatter(slot, j):
        return pltpu.make_async_remote_copy(
            xs.at[slot + 1, piece_rows(j)],
            out.at[0, u],
            out_send.at[slot, j],
            out_recv.at[u],
            device_id={"section": 2 * k + slot, "tm": 4 * c + j},
            device_id_type=MESH,
        )

    def scatter_local(slot, j):
        return pltpu.make_async_copy(xs.at[slot + 1, piece_rows(j)], out.at[0, u], out_recv.at[u])

    def own_piece(slot, j):
        return (slot == c) & (4 * c + j == t)

    own = pl.ds(pl.multiple_of(c * ROWS, ROWS), ROWS)

    def kv_part(slot, i, rows):
        ref = kv.at[slot, i // 2, rows, pl.ds((i % 2) * 512, 512)]
        return pltpu.make_async_remote_copy(
            ref, ref, kv_send.at[slot, i], kv_recv.at[slot, i], device_id=partner, device_id_type=MESH
        )

    def kv_copy(slot, i):
        return kv_part(slot, i, own)

    def kv_arrival(slot, i):
        return kv_part(slot, i, pl.ds(pl.multiple_of((1 - c) * ROWS, ROWS), ROWS))

    def hand_over():
        return pltpu.make_async_remote_copy(
            depth, res, hand_send, hand_recv, device_id=partner, device_id_type=MESH
        )

    def rim_copy(slot):
        return pltpu.make_async_remote_copy(
            rim_out.at[slot],
            rim_in.at[slot],
            rim_send.at[slot],
            rim_recv.at[slot],
            device_id=partner,
            device_id_type=MESH,
        )

    def run_slot(slot, carry):
        mine = slot == c

        def ready(*ids):
            for i in ids:

                @pl.when(mine)
                def _(i=i):
                    local(i).wait()

                @pl.when(jnp.logical_not(mine))
                def _(i=i):
                    pull(i, slot).wait_recv()

        length = lengths[u]

        def input_ready(j):
            itself = lead & (j == t) & (t < 4)

            @pl.when(itself)
            def _():
                frame_local(u).wait()

            @pl.when(jnp.logical_not(itself))
            def _():
                pltpu.make_async_remote_copy(
                    first_piece, first_piece, x_send.at[0], x_recv.at[j], device_id=partner, device_id_type=MESH
                ).wait_recv()

        opening = (k == 0) & (slot == 0)
        passes = jnp.where(opening, jnp.where(c == 0, 4, 0), 2)

        @pl.when(jnp.logical_not(opening & (c == 1)))
        def _():
            ready(0, 7, 8)

        def feed_forward(i, carry):
            group = i // 2
            source = xs.at[slot + group]
            rows = pl.ds(pl.multiple_of(lax.rem(i, 2) * HALF, HALF), HALF)

            @pl.when(slot == 0)
            def _():
                input_ready(2 * i)
                input_ready(2 * i + 1)

            act[rows] = normed(source[rows].astype(F32), vec[slot, 0]).astype(BF16)
            for n in range(4):
                cols = pl.ds(n * 512, 512)
                v = dot(act[rows], w_up[slot, :, cols])
                wide[rows, cols] = (v * sigmoid(v)).astype(BF16)
            for n in range(2):
                cols = pl.ds(n * 512, 512)
                v = dot(wide[rows], w_down[slot, :, cols])
                sums[group, rows, cols] = source[rows, cols].astype(F32) + 0.5 * v
            return carry

        lax.fori_loop(0, passes, feed_forward, 0)

        @pl.when(opening & (c == 0))
        def _():
            hand_over().start()

        @pl.when(opening & (c == 1))
        def _():
            hand_over().wait_recv()

        ready(1, 9, 10)
        act[...] = normed(res[...], vec[slot, 1]).astype(BF16)
        for i in range(4):
            cols = pl.ds((i // 2) * 512, 512)
            w = (w_key, w_value)[i % 2]
            kv[slot, i % 2, own, cols] = dot(act[...], w[slot, :, cols]).astype(BF16)
            kv_copy(slot, 2 * (i % 2) + i // 2).start()
        ready(11)
        for n in range(2):
            cols = pl.ds(n * 512, 512)
            wide[:, cols] = (dot(act[...], w_query[slot, :, cols]) * QUERY_SCALE).astype(BF16)
        kv_arrival(slot, 0).wait_recv()
        kv_arrival(slot, 2).wait_recv()

        low = lax.broadcasted_iota(jnp.int32, (ROWS, 128), 1) < 64
        one = jnp.where(lax.broadcasted_iota(jnp.int32, (ROWS, 128), 1) == 0, 1.0, 0.0).astype(BF16)
        ones = jnp.ones((LEN, 128), BF16)

        def pair_scores(g):
            cols = pl.ds(g * 128, 128)
            q = wide[:, cols]
            none = jnp.zeros_like(q)
            stacked = jnp.concatenate(
                [
                    jnp.concatenate([jnp.where(low, q, none), one], axis=1),
                    jnp.concatenate([jnp.where(low, none, q), one], axis=1),
                ],
                axis=0,
            )
            keys = jnp.concatenate([kv[slot, 0, :, cols], bias[...]], axis=1)
            return lax.dot_general(
                stacked, keys, (((1,), (1,)), ((), ())), preferred_element_type=F32
            )

        def pair_context(g, scores):
            cols = pl.ds(g * 128, 128)
            peak = jnp.max(scores, axis=-1, keepdims=True)
            weights = jnp.exp2(scores - peak).astype(BF16)
            values = jnp.concatenate([kv[slot, 1, :, cols], ones], axis=1)
            mixed = dot(weights, values)
            total = jnp.where(low, mixed[:ROWS, 128:], mixed[ROWS:, 128:])
            mixed = jnp.where(low, mixed[:ROWS, :128], mixed[ROWS:, :128])
            act[:, cols] = (mixed / total).astype(BF16)

        scores = pair_scores(0)
        for g in range(HEADS // 2):
            if g == 3:
                kv_arrival(slot, 1).wait_recv()
                kv_arrival(slot, 3).wait_recv()
            later = pair_scores(g + 1) if g + 1 < HEADS // 2 else None
            pair_context(g, scores)
            scores = later
        ready(12)

        def out_tile(n):
            cols = pl.ds(n * 512, 512)
            res[:, cols] = res[:, cols] + dot(act[...], w_out[slot, :, cols])

        for n in range(2):
            out_tile(n)
        ready(2, 13, 6)

        @pl.when(opening & (c == 0))
        def _():
            hand_over().wait_send()

        wide[:, :D] = normed(res[...], vec[slot, 2]).astype(BF16)
        row = c * ROWS + lax.broadcasted_iota(jnp.int32, (ROWS, 256), 0)
        keep = (row < length).astype(F32)

        def glu_tile(n):
            value = dot(wide[:, :D], w_expand[slot, :, pl.ds(n * 256, 256)])
            gate = dot(wide[:, :D], w_expand[slot, :, pl.ds(n * 256 + D, 256)])
            glu = (value * sigmoid(gate) * keep).astype(BF16)
            rim_out[slot, :, pl.ds(n * 256, 256)] = jnp.where(c == 0, glu[ROWS - 16 :], glu[:16])
            glu = glu.astype(F32)
            padded[2 * n, pl.ds(16, ROWS), :] = glu[:, :128]
            padded[2 * n + 1, pl.ds(16, ROWS), :] = glu[:, 128:]

        def conv_rows(n, base, blocks):
            cols = pl.ds(n * 128, 128)
            weights = [taps[slot, pl.ds(j, 1), cols] for j in range(TAPS)]
            total = [None] * blocks
            for o in range(1, 8 * (blocks - 1) + TAPS + 1):
                v = padded[n, pl.ds(base + o, 8), :]
                for b in range(blocks):
                    j = o - 1 - 8 * b
                    if 0 <= j < TAPS:
                        term = v * weights[j]
                        total[b] = term if total[b] is None else total[b] + term
            for b in range(blocks):
                depth[pl.ds(base + 8 * b, 8), cols] = total[b]

        for n in range(5):
            if n < 4:
                glu_tile(n)
            if n == 3:
                rim_copy(slot).start()
            if n > 0:
                for i in (2 * n - 2, 2 * n - 1):
                    conv_rows(i, 0, 16)
                    conv_rows(i, 128, 16)
        ready(3, 4)
        rim_copy(slot).wait_recv()
        inner_rim = pl.ds(pl.multiple_of((1 - c) * (ROWS + 16), 16), 16)
        edge = pl.multiple_of((1 - c) * (ROWS - 16), 16)
        for n in range(8):
            padded[n, inner_rim, :] = rim_in[slot, :, n * 128 : (n + 1) * 128].astype(F32)
            conv_rows(n, edge, 2)
        ready(14, 5)
        for h in range(2):
            rows = pl.ds(h * HALF, HALF)
            shifted = normed(depth[rows], vec[slot, 3]) + vec[slot, 4]
            act[rows] = (shifted * sigmoid(shifted)).astype(BF16)
            closing = res[rows] + dot(act[rows], w_shrink[slot])
            xs[slot + 1, rows] = normed(closing, vec[slot, 5]).astype(BF16)
            for j in (2 * h, 2 * h + 1):

                @pl.when((slot == 1) & (k < STAGES - 1))
                def _(j=j):
                    if j == 0:

                        @pl.when(even)
                        def _():
                            leave_x().start()

                        @pl.when(jnp.logical_not(even))
                        def _():
                            leave_z().start()

                    else:
                        forward(j).start()

                @pl.when(own_piece(slot, j))
                def _(j=j):
                    scatter_local(slot, j).start()

                @pl.when(jnp.logical_not(own_piece(slot, j)))
                def _(j=j):
                    scatter(slot, j).start()

        return carry

    @pl.when(active)
    def _():
        seen = lax.broadcasted_iota(jnp.int32, (LEN, 128), 0) < lengths[u]
        bias[...] = jnp.where(seen, 0.0, -1e30).astype(BF16)
        for n in range(8):
            padded[n, pl.ds(0, 16), :] = jnp.zeros((16, 128), F32)
            padded[n, pl.ds(16 + ROWS, 16), :] = jnp.zeros((16, 128), F32)
        lax.fori_loop(0, 2, run_slot, 0)
        for i in ORDER:

            @pl.when(pushed(i))
            def _(i=i):
                push(i).wait_send()

        for slot in range(2):
            for i in range(4):
                kv_copy(slot, i).wait_send()
            rim_copy(slot).wait_send()
            for j in range(PIECES):

                @pl.when(jnp.logical_not(own_piece(slot, j)))
                def _(slot=slot, j=j):
                    scatter(slot, j).wait_send()

        @pl.when(k < STAGES - 1)
        def _():
            for j in range(PIECES):
                forward(j).wait_send()

    for v in range(UTTS):

        @pl.when(sends_frames & jnp.logical_not((c == 0) & (t == 2 * v + 1)))
        def _(v=v):
            frame_copy(v).wait_send()

    for v in range(UTTS):
        itself = (t == 2 * v + side) & (c == t // 4)
        landed = out.at[0, v]

        @pl.when(itself)
        def _(v=v, landed=landed):
            pltpu.make_async_copy(xs.at[0, piece_rows(0)], landed, out_recv.at[v]).wait()

        @pl.when(jnp.logical_not(itself))
        def _(v=v, landed=landed):
            pltpu.make_async_remote_copy(
                landed, landed, out_send.at[0, 0], out_recv.at[v], device_id=partner, device_id_type=MESH
            ).wait_recv()


def body(
    frames,
    lengths,
    ffn_gain,
    ffn_up,
    ffn_down,
    attn_gain,
    query_weight,
    key_weight,
    value_weight,
    out_weight,
    conv_gain,
    expand_weight,
    depth_weight,
    depth_gain,
    norm_shift,
    shrink_weight,
    final_gain,
):
    anywhere = pl.BlockSpec(memory_space=pl.ANY)
    dma = pltpu.SemaphoreType.DMA
    return pl.pallas_call(
        block_kernel,
        name="conformer",
        out_shape=jax.ShapeDtypeStruct((1, UTTS, PIECE, D), BF16),
        in_specs=[pl.BlockSpec(memory_space=pltpu.SMEM)] + [anywhere] * 16,
        out_specs=anywhere,
        scratch_shapes=[pltpu.VMEM((2,) + shape, BF16) for shape in SHAPES]
        + [
            pltpu.VMEM((2, 6, 1, D), F32),
            pltpu.VMEM((2, TAPS, D), F32),
            pltpu.VMEM((3, ROWS, D), BF16),
            pltpu.VMEM((ROWS, D), BF16),
            pltpu.VMEM((ROWS, FF), BF16),
            pltpu.VMEM((2, ROWS, D), F32),
            pltpu.VMEM((2, 2, LEN, D), BF16),
            pltpu.VMEM((2, 16, D), BF16),
            pltpu.VMEM((2, 16, D), BF16),
            pltpu.VMEM((LEN, 128), BF16),
            pltpu.VMEM((8, ROWS + 32, 128), F32),
            pltpu.VMEM((PIECE, D), BF16),
            pltpu.VMEM((PIECE, D), BF16),
            dma((15,)),
            dma((15,)),
            dma((15,)),
            dma((PIECES,)),
            dma((2 * PIECES,)),
            dma((2, PIECES)),
            dma((UTTS,)),
            dma((2, 4)),
            dma((2, 4)),
            dma((2,)),
            dma((2,)),
            dma((UTTS,)),
            dma((2,)),
            dma((2,)),
            dma,
            dma,
        ],
        compiler_params=pltpu.CompilerParams(
            has_side_effects=True, vmem_limit_bytes=67043328
        ),
    )(
        lengths,
        frames,
        ffn_gain,
        attn_gain,
        conv_gain,
        depth_gain,
        norm_shift,
        final_gain,
        depth_weight,
        ffn_up,
        ffn_down,
        key_weight,
        value_weight,
        query_weight,
        out_weight,
        expand_weight,
        shrink_weight,
    )


def solution(mesh):
    return jax.shard_map(
        body,
        mesh=mesh,
        in_specs=(
            P(None, "tm", None),
            P(),
            P("section", None),
            P("section", None, None),
            P("section", None, None),
            P("section", None),
            P("section", None, None),
            P("section", None, None),
            P("section", None, None),
            P("section", None, None),
            P("section", None),
            P("section", None, None),
            P("section", None, None),
            P("section", None),
            P("section", None),
            P("section", None, None),
            P("section", None),
        ),
        out_specs=P("section", None, "tm", None),
        check_vma=False,
    )
```

```python
import functools

import jax
import jax.numpy as jnp
from jax import lax
from jax.experimental import pallas as pl
from jax.experimental.pallas import tpu as pltpu
from jax.sharding import PartitionSpec as P

MESH = pl.DeviceIdType.MESH
F32 = jnp.float32
BF16 = jnp.bfloat16
EPS = 1e-05
D = 1024
FF = 2048
HEADS = 16
ROWS = 256
LEN = 512
TAPS = 31
UTTS = 4
STAGES = 8
PIECE = 64
PIECES = ROWS // PIECE
HALF = ROWS // 2
QUERY_SCALE = 0.125 * 1.4426950408889634
SHAPES = ((D, FF), (FF, D), (D, D), (D, D), (D, D), (D, D), (D, 2 * D), (D, D))


def sigmoid(v):
    return 0.5 * jnp.tanh(0.5 * v) + 0.5


def normed(v, gain):
    mean = jnp.mean(v, axis=-1, keepdims=True)
    centred = v - mean
    spread = jnp.mean(centred * centred, axis=-1, keepdims=True)
    return centred * lax.rsqrt(spread + EPS) * gain


def dot(a, b):
    return jnp.dot(a, b, preferred_element_type=F32)


def block_kernel(
    lengths,
    frames,
    ffn_gain,
    attn_gain,
    conv_gain,
    depth_gain,
    norm_shift,
    final_gain,
    depth_weight,
    h_up,
    h_down,
    h_key,
    h_value,
    h_query,
    h_out,
    h_expand,
    h_shrink,
    out,
    w_up,
    w_down,
    w_key,
    w_value,
    w_query,
    w_out,
    w_expand,
    w_shrink,
    vec,
    taps,
    xs,
    act,
    wide,
    sums,
    kv,
    rim_out,
    rim_in,
    bias,
    padded,
    via_z,
    local_sem,
    push_sem,
    pull_sem,
    x_send,
    x_recv,
    out_send,
    out_recv,
    kv_send,
    kv_recv,
    rim_send,
    rim_recv,
    frame_send,
    via_send,
    via_recv,
    hand_send,
    hand_recv,
):
    res, depth = sums.at[0], sums.at[1]
    s = lax.axis_index("section")
    t = lax.axis_index("tm")
    k = s // 2
    c = lax.rem(s, 2)
    u = t // 2
    side = 1 - lax.rem(k, 2)
    active = lax.rem(t, 2) == side
    partner = {"section": 2 * k + 1 - c, "tm": t}
    here = {"section": s, "tm": t}
    del here

    hbm = (h_up, h_down, h_key, h_value, h_query, h_out, h_expand, h_shrink)
    vmem = (w_up, w_down, w_key, w_value, w_query, w_out, w_expand, w_shrink)
    small = (ffn_gain, attn_gain, conv_gain, depth_gain, norm_shift, final_gain)

    def sources():
        pairs = [(small[i], vec.at[c, i]) for i in range(6)]
        pairs += [(depth_weight, taps.at[c])]
        pairs += [(hbm[i].at[0], vmem[i].at[c]) for i in range(8)]
        return pairs

    def arrivals(slot):
        refs = [vec.at[slot, i] for i in range(6)] + [taps.at[slot]]
        return refs + [vmem[i].at[slot] for i in range(8)]

    def local(i):
        src, dst = sources()[i]
        return pltpu.make_async_copy(src, dst, local_sem.at[i])

    def push(i):
        src, dst = sources()[i]
        return pltpu.make_async_remote_copy(
            src, dst, push_sem.at[i], pull_sem.at[i], device_id=partner, device_id_type=MESH
        )

    def pull(i, slot):
        ref = arrivals(slot)[i]
        return pltpu.make_async_remote_copy(
            ref, ref, push_sem.at[i], pull_sem.at[i], device_id=partner, device_id_type=MESH
        )

    lead = (k == 0) & (c == 0)

    def pushed(i):
        return jnp.logical_not(lead) if i in (0, 7, 8) else k >= 0

    ORDER = (0, 7, 8, 1, 9, 10, 11, 12, 2, 6, 13, 3, 4, 14, 5)


    frame_rows = xs.at[t // 4, pl.ds(pl.multiple_of(lax.rem(t, 4) * PIECE, PIECE), PIECE)]

    def frame_copy(v):
        return pltpu.make_async_remote_copy(
            frames.at[v],
            frame_rows,
            frame_send.at[v],
            x_recv.at[t],
            device_id={"section": 0, "tm": 2 * v + 1},
            device_id_type=MESH,
        )

    def frame_local(v):
        return pltpu.make_async_copy(frames.at[v], frame_rows, x_recv.at[t])

    sends_frames = (k == 0) & (t // 4 == c)
    for v in range(UTTS):
        to_itself = (c == 0) & (t == 2 * v + 1)

        @pl.when(sends_frames & jnp.logical_not(to_itself))
        def _(v=v):
            frame_copy(v).start()

        @pl.when(sends_frames & to_itself)
        def _(v=v):
            frame_local(v).start()

    LEAD = ((1, 9, 10, 11), (12, 2, 6, 13), (3, 4, 14, 5))
    MATE = ((0, 7, 8), (1, 9, 10), (11, 12, 2, 6, 13, 3, 4, 14, 5))

    def push_part(part, first):
        @pl.when(first & (c == 0))
        def _():
            for i in LEAD[part]:
                push(i).start()

        @pl.when(first & (c == 1))
        def _():
            for i in MATE[part]:
                push(i).start()

    @pl.when(active)
    def _():
        for i in ORDER:
            local(i).start()
        push_part(0, k == 0)

        @pl.when(k > 0)
        def _():
            for i in ORDER:
                push(i).start()

    def piece_rows(j):
        return pl.ds(j * PIECE, PIECE)

    def forward(j):
        return pltpu.make_async_remote_copy(
            xs.at[2, piece_rows(j)],
            xs.at[0, piece_rows(j)],
            x_send.at[j],
            x_recv.at[j],
            device_id={"section": lax.rem(s + 2, 16), "tm": 2 * u + 1 - side},
            device_id_type=MESH,
        )

    def relayed(src, dst, send, recv, section, tm):
        return pltpu.make_async_remote_copy(
            src, dst, send, recv, device_id={"section": lax.rem(section + 16, 16), "tm": tm}, device_id_type=MESH
        )

    even = lax.rem(k, 2) == 0
    first_piece = xs.at[0, pl.ds(0, PIECE)]
    last_first = xs.at[2, pl.ds(0, PIECE)]

    def leave_z():
        return relayed(last_first, via_z, x_send.at[0], via_recv, s + 4, 2 * u + 1)

    def land_z():
        return relayed(via_z, first_piece, via_send, x_recv.at[0], s - 2, 2 * u + 1)

    idle = jnp.logical_not(active)

    @pl.when(idle & jnp.logical_not(even) & (k >= 3))
    def _():
        leave_z().wait_recv()
        land_z().start()
        land_z().wait_send()

    def scatter(slot, j):
        return pltpu.make_async_remote_copy(
            xs.at[slot + 1, piece_rows(j)],
            out.at[0, u],
            out_send.at[slot, j],
            out_recv.at[u],
            device_id={"section": 2 * k + slot, "tm": 4 * c + j},
            device_id_type=MESH,
        )

    def scatter_local(slot, j):
        return pltpu.make_async_copy(xs.at[slot + 1, piece_rows(j)], out.at[0, u], out_recv.at[u])

    def own_piece(slot, j):
        return (slot == c) & (4 * c + j == t)

    def emit(slot, j):
        @pl.when(own_piece(slot, j))
        def _():
            scatter_local(slot, j).start()

        @pl.when(jnp.logical_not(own_piece(slot, j)))
        def _():
            scatter(slot, j).start()

    own = pl.ds(pl.multiple_of(c * ROWS, ROWS), ROWS)

    def kv_part(slot, i, rows):
        ref = kv.at[slot, i // 2, rows, pl.ds((i % 2) * 512, 512)]
        return pltpu.make_async_remote_copy(
            ref, ref, kv_send.at[slot, i], kv_recv.at[slot, i], device_id=partner, device_id_type=MESH
        )

    def kv_copy(slot, i):
        return kv_part(slot, i, own)

    def kv_arrival(slot, i):
        return kv_part(slot, i, pl.ds(pl.multiple_of((1 - c) * ROWS, ROWS), ROWS))

    def hand_over():
        return pltpu.make_async_remote_copy(
            depth, res, hand_send, hand_recv, device_id=partner, device_id_type=MESH
        )

    def rim_copy(slot):
        return pltpu.make_async_remote_copy(
            rim_out.at[slot],
            rim_in.at[slot],
            rim_send.at[slot],
            rim_recv.at[slot],
            device_id=partner,
            device_id_type=MESH,
        )

    def run_slot(slot, carry):
        mine = slot == c

        def ready(*ids):
            for i in ids:

                @pl.when(mine)
                def _(i=i):
                    local(i).wait()

                @pl.when(jnp.logical_not(mine))
                def _(i=i):
                    pull(i, slot).wait_recv()

        length = lengths[u]

        def input_ready(j):
            itself = lead & (j == t) & (t < 4)

            @pl.when(itself)
            def _():
                frame_local(u).wait()

            @pl.when(jnp.logical_not(itself))
            def _():
                pltpu.make_async_remote_copy(
                    first_piece, first_piece, x_send.at[0], x_recv.at[j], device_id=partner, device_id_type=MESH
                ).wait_recv()

        opening = (k == 0) & (slot == 0)
        passes = jnp.where(opening, jnp.where(c == 0, 4, 0), 2)

        @pl.when(jnp.logical_not(opening & (c == 1)))
        def _():
            ready(0, 7, 8)

        def feed_forward(i, carry):
            group = i // 2
            source = xs.at[slot + group]
            rows = pl.ds(pl.multiple_of(lax.rem(i, 2) * HALF, HALF), HALF)

            @pl.when(slot == 0)
            def _():
                input_ready(2 * i)
                input_ready(2 * i + 1)

            act[rows] = normed(source[rows].astype(F32), vec[slot, 0]).astype(BF16)
            for n in range(4):
                cols = pl.ds(n * 512, 512)
                v = dot(act[rows], w_up[slot, :, cols])
                wide[rows, cols] = (v * sigmoid(v)).astype(BF16)
            for n in range(2):
                cols = pl.ds(n * 512, 512)
                v = dot(wide[rows], w_down[slot, :, cols])
                sums[group, rows, cols] = source[rows, cols].astype(F32) + 0.5 * v
            return carry

        lax.fori_loop(0, passes, feed_forward, 0)

        @pl.when(opening & (c == 0))
        def _():
            hand_over().start()

        @pl.when(opening & (c == 1))
        def _():
            hand_over().wait_recv()

        ready(1, 9, 10)
        act[...] = normed(res[...], vec[slot, 1]).astype(BF16)
        for i in range(4):
            cols = pl.ds((i // 2) * 512, 512)
            w = (w_key, w_value)[i % 2]
            kv[slot, i % 2, own, cols] = dot(act[...], w[slot, :, cols]).astype(BF16)
            kv_copy(slot, 2 * (i % 2) + i // 2).start()
        push_part(1, opening)

        @pl.when(slot == 1)
        def _():
            for j in range(PIECES):
                emit(0, j)

        ready(11)
        for n in range(2):
            cols = pl.ds(n * 512, 512)
            wide[:, cols] = (dot(act[...], w_query[slot, :, cols]) * QUERY_SCALE).astype(BF16)
        kv_arrival(slot, 0).wait_recv()
        kv_arrival(slot, 2).wait_recv()

        low = lax.broadcasted_iota(jnp.int32, (ROWS, 128), 1) < 64
        one = jnp.where(lax.broadcasted_iota(jnp.int32, (ROWS, 128), 1) == 0, 1.0, 0.0).astype(BF16)
        ones = jnp.ones((LEN, 128), BF16)

        def pair_scores(g):
            cols = pl.ds(g * 128, 128)
            q = wide[:, cols]
            none = jnp.zeros_like(q)
            stacked = jnp.concatenate(
                [
                    jnp.concatenate([jnp.where(low, q, none), one], axis=1),
                    jnp.concatenate([jnp.where(low, none, q), one], axis=1),
                ],
                axis=0,
            )
            keys = jnp.concatenate([kv[slot, 0, :, cols], bias[...]], axis=1)
            return lax.dot_general(
                stacked, keys, (((1,), (1,)), ((), ())), preferred_element_type=F32
            )

        def pair_context(g, scores):
            cols = pl.ds(g * 128, 128)
            peak = jnp.max(scores, axis=-1, keepdims=True)
            weights = jnp.exp2(scores - peak).astype(BF16)
            values = jnp.concatenate([kv[slot, 1, :, cols], ones], axis=1)
            mixed = dot(weights, values)
            total = jnp.where(low, mixed[:ROWS, 128:], mixed[ROWS:, 128:])
            mixed = jnp.where(low, mixed[:ROWS, :128], mixed[ROWS:, :128])
            act[:, cols] = (mixed / total).astype(BF16)

        scores = pair_scores(0)
        for g in range(HEADS // 2):
            if g == 3:
                kv_arrival(slot, 1).wait_recv()
                kv_arrival(slot, 3).wait_recv()
            later = pair_scores(g + 1) if g + 1 < HEADS // 2 else None
            pair_context(g, scores)
            scores = later
        ready(12)

        def out_tile(n):
            cols = pl.ds(n * 512, 512)
            res[:, cols] = res[:, cols] + dot(act[...], w_out[slot, :, cols])

        for n in range(2):
            out_tile(n)
        ready(2, 13, 6)

        @pl.when(opening & (c == 0))
        def _():
            hand_over().wait_send()

        wide[:, :D] = normed(res[...], vec[slot, 2]).astype(BF16)
        row = c * ROWS + lax.broadcasted_iota(jnp.int32, (ROWS, 256), 0)
        keep = (row < length).astype(F32)

        def glu_tile(n):
            value = dot(wide[:, :D], w_expand[slot, :, pl.ds(n * 256, 256)])
            gate = dot(wide[:, :D], w_expand[slot, :, pl.ds(n * 256 + D, 256)])
            glu = (value * sigmoid(gate) * keep).astype(BF16)
            rim_out[slot, :, pl.ds(n * 256, 256)] = jnp.where(c == 0, glu[ROWS - 16 :], glu[:16])
            glu = glu.astype(F32)
            padded[2 * n, pl.ds(16, ROWS), :] = glu[:, :128]
            padded[2 * n + 1, pl.ds(16, ROWS), :] = glu[:, 128:]

        def conv_rows(n, base, blocks):
            cols = pl.ds(n * 128, 128)
            weights = [taps[slot, j, :, cols] for j in range(TAPS)]
            total = [None] * blocks
            for o in range(1, 8 * (blocks - 1) + TAPS + 1):
                v = padded[n, pl.ds(base + o, 8), :]
                for b in range(blocks):
                    j = o - 1 - 8 * b
                    if 0 <= j < TAPS:
                        term = v * weights[j]
                        total[b] = term if total[b] is None else total[b] + term
            for b in range(blocks):
                depth[pl.ds(base + 8 * b, 8), cols] = total[b]

        for n in range(5):
            if n < 4:
                glu_tile(n)
            if n == 3:
                rim_copy(slot).start()
                push_part(2, opening)
            if n > 0:
                for i in (2 * n - 2, 2 * n - 1):
                    conv_rows(i, 0, 16)
                    conv_rows(i, 128, 16)
        ready(3, 4)
        rim_copy(slot).wait_recv()
        inner_rim = pl.ds(pl.multiple_of((1 - c) * (ROWS + 16), 16), 16)
        edge = pl.multiple_of((1 - c) * (ROWS - 16), 16)
        for n in range(8):
            padded[n, inner_rim, :] = rim_in[slot, :, n * 128 : (n + 1) * 128].astype(F32)
            conv_rows(n, edge, 2)
        ready(14, 5)
        for h in range(2):
            rows = pl.ds(h * HALF, HALF)
            shifted = normed(depth[rows], vec[slot, 3]) + vec[slot, 4]
            act[rows] = (shifted * sigmoid(shifted)).astype(BF16)
            closing = res[rows] + dot(act[rows], w_shrink[slot])
            xs[slot + 1, rows] = normed(closing, vec[slot, 5]).astype(BF16)
            for j in (2 * h, 2 * h + 1):

                @pl.when((slot == 1) & (k < STAGES - 1))
                def _(j=j):
                    if j == 0:

                        @pl.when(even)
                        def _():
                            forward(0).start()

                        @pl.when(jnp.logical_not(even))
                        def _():
                            leave_z().start()

                    else:
                        forward(j).start()

                @pl.when((slot == 1) & (k == STAGES - 1))
                def _(j=j):
                    emit(1, j)

        @pl.when((slot == 1) & (k < STAGES - 1))
        def _():
            for j in range(PIECES):
                emit(1, j)

        return carry

    @pl.when(active)
    def _():
        seen = lax.broadcasted_iota(jnp.int32, (LEN, 128), 0) < lengths[u]
        bias[...] = jnp.where(seen, 0.0, -1e30).astype(BF16)
        for n in range(8):
            padded[n, pl.ds(0, 16), :] = jnp.zeros((16, 128), F32)
            padded[n, pl.ds(16 + ROWS, 16), :] = jnp.zeros((16, 128), F32)
        lax.fori_loop(0, 2, run_slot, 0)
        for i in ORDER:

            @pl.when(pushed(i))
            def _(i=i):
                push(i).wait_send()

        for slot in range(2):
            for i in range(4):
                kv_copy(slot, i).wait_send()
            rim_copy(slot).wait_send()
            for j in range(PIECES):

                @pl.when(jnp.logical_not(own_piece(slot, j)))
                def _(slot=slot, j=j):
                    scatter(slot, j).wait_send()

        @pl.when(k < STAGES - 1)
        def _():
            for j in range(PIECES):
                forward(j).wait_send()

    for v in range(UTTS):

        @pl.when(sends_frames & jnp.logical_not((c == 0) & (t == 2 * v + 1)))
        def _(v=v):
            frame_copy(v).wait_send()

    for v in range(UTTS):
        itself = (t == 2 * v + side) & (c == t // 4)
        landed = out.at[0, v]

        @pl.when(itself)
        def _(v=v, landed=landed):
            pltpu.make_async_copy(xs.at[0, piece_rows(0)], landed, out_recv.at[v]).wait()

        @pl.when(jnp.logical_not(itself))
        def _(v=v, landed=landed):
            pltpu.make_async_remote_copy(
                landed, landed, out_send.at[0, 0], out_recv.at[v], device_id=partner, device_id_type=MESH
            ).wait_recv()


def body(
    frames,
    lengths,
    ffn_gain,
    ffn_up,
    ffn_down,
    attn_gain,
    query_weight,
    key_weight,
    value_weight,
    out_weight,
    conv_gain,
    expand_weight,
    depth_weight,
    depth_gain,
    norm_shift,
    shrink_weight,
    final_gain,
):
    anywhere = pl.BlockSpec(memory_space=pl.ANY)
    dma = pltpu.SemaphoreType.DMA
    return pl.pallas_call(
        block_kernel,
        name="conformer",
        out_shape=jax.ShapeDtypeStruct((1, UTTS, PIECE, D), BF16),
        in_specs=[pl.BlockSpec(memory_space=pltpu.SMEM)] + [anywhere] * 16,
        out_specs=anywhere,
        scratch_shapes=[pltpu.VMEM((2,) + shape, BF16) for shape in SHAPES]
        + [
            pltpu.VMEM((2, 6, 1, D), F32),
            pltpu.VMEM((2, TAPS, 1, D), F32),
            pltpu.VMEM((3, ROWS, D), BF16),
            pltpu.VMEM((ROWS, D), BF16),
            pltpu.VMEM((ROWS, FF), BF16),
            pltpu.VMEM((2, ROWS, D), F32),
            pltpu.VMEM((2, 2, LEN, D), BF16),
            pltpu.VMEM((2, 16, D), BF16),
            pltpu.VMEM((2, 16, D), BF16),
            pltpu.VMEM((LEN, 128), BF16),
            pltpu.VMEM((8, ROWS + 32, 128), F32),
            pltpu.VMEM((PIECE, D), BF16),
            dma((15,)),
            dma((15,)),
            dma((15,)),
            dma((PIECES,)),
            dma((2 * PIECES,)),
            dma((2, PIECES)),
            dma((UTTS,)),
            dma((2, 4)),
            dma((2, 4)),
            dma((2,)),
            dma((2,)),
            dma((UTTS,)),
            dma,
            dma,
            dma,
            dma,
        ],
        compiler_params=pltpu.CompilerParams(
            has_side_effects=True, vmem_limit_bytes=67043328
        ),
    )(
        lengths,
        frames,
        ffn_gain,
        attn_gain,
        conv_gain,
        depth_gain,
        norm_shift,
        final_gain,
        jnp.transpose(depth_weight, (1, 0, 2)),
        ffn_up,
        ffn_down,
        key_weight,
        value_weight,
        query_weight,
        out_weight,
        expand_weight,
        shrink_weight,
    )


def solution(mesh):
    return jax.shard_map(
        body,
        mesh=mesh,
        in_specs=(
            P(None, "tm", None),
            P(),
            P("section", None),
            P("section", None, None),
            P("section", None, None),
            P("section", None),
            P("section", None, None),
            P("section", None, None),
            P("section", None, None),
            P("section", None, None),
            P("section", None),
            P("section", None, None),
            P("section", None, None),
            P("section", None),
            P("section", None),
            P("section", None, None),
            P("section", None),
        ),
        out_specs=P("section", None, "tm", None),
        check_vma=False,
    )
```

```python
import functools

import jax
import jax.numpy as jnp
from jax import lax
from jax.experimental import pallas as pl
from jax.experimental.pallas import tpu as pltpu
from jax.sharding import PartitionSpec as P

MESH = pl.DeviceIdType.MESH
F32 = jnp.float32
BF16 = jnp.bfloat16
EPS = 1e-05
D = 1024
FF = 2048
HEADS = 16
ROWS = 256
LEN = 512
TAPS = 31
UTTS = 4
STAGES = 8
PIECE = 64
PIECES = ROWS // PIECE
HALF = ROWS // 2
QUERY_SCALE = 0.125 * 1.4426950408889634
SHAPES = ((D, FF), (FF, D), (D, D), (D, D), (D, D), (D, D), (D, 2 * D), (D, D))


def sigmoid(v):
    return 0.5 * jnp.tanh(0.5 * v) + 0.5


def normed(v, gain):
    mean = jnp.mean(v, axis=-1, keepdims=True)
    centred = v - mean
    spread = jnp.mean(centred * centred, axis=-1, keepdims=True)
    return centred * lax.rsqrt(spread + EPS) * gain


def dot(a, b):
    return jnp.dot(a, b, preferred_element_type=F32)


def block_kernel(
    lengths,
    frames,
    ffn_gain,
    attn_gain,
    conv_gain,
    depth_gain,
    norm_shift,
    final_gain,
    depth_weight,
    h_up,
    h_down,
    h_key,
    h_value,
    h_query,
    h_out,
    h_expand,
    h_shrink,
    out,
    w_up,
    w_down,
    w_key,
    w_value,
    w_query,
    w_out,
    w_expand,
    w_shrink,
    vec,
    taps,
    xs,
    act,
    wide,
    sums,
    kv,
    rim_out,
    rim_in,
    bias,
    padded,
    via_z,
    local_sem,
    push_sem,
    pull_sem,
    x_send,
    x_recv,
    out_send,
    out_recv,
    kv_send,
    kv_recv,
    rim_send,
    rim_recv,
    frame_send,
    via_send,
    via_recv,
    hand_send,
    hand_recv,
):
    res, depth = sums.at[0], sums.at[1]
    s = lax.axis_index("section")
    t = lax.axis_index("tm")
    k = s // 2
    c = lax.rem(s, 2)
    u = t // 2
    side = 1 - lax.rem(k, 2)
    active = lax.rem(t, 2) == side
    partner = {"section": 2 * k + 1 - c, "tm": t}
    here = {"section": s, "tm": t}
    del here

    hbm = (h_up, h_down, h_key, h_value, h_query, h_out, h_expand, h_shrink)
    vmem = (w_up, w_down, w_key, w_value, w_query, w_out, w_expand, w_shrink)
    small = (ffn_gain, attn_gain, conv_gain, depth_gain, norm_shift, final_gain)

    def sources():
        pairs = [(small[i], vec.at[c, i]) for i in range(6)]
        pairs += [(depth_weight, taps.at[c])]
        pairs += [(hbm[i].at[0], vmem[i].at[c]) for i in range(8)]
        return pairs

    def arrivals(slot):
        refs = [vec.at[slot, i] for i in range(6)] + [taps.at[slot]]
        return refs + [vmem[i].at[slot] for i in range(8)]

    def local(i):
        src, dst = sources()[i]
        return pltpu.make_async_copy(src, dst, local_sem.at[i])

    def push(i):
        src, dst = sources()[i]
        return pltpu.make_async_remote_copy(
            src, dst, push_sem.at[i], pull_sem.at[i], device_id=partner, device_id_type=MESH
        )

    def pull(i, slot):
        ref = arrivals(slot)[i]
        return pltpu.make_async_remote_copy(
            ref, ref, push_sem.at[i], pull_sem.at[i], device_id=partner, device_id_type=MESH
        )

    lead = (k == 0) & (c == 0)

    def pushed(i):
        return jnp.logical_not(lead) if i in (0, 7, 8) else k >= 0

    ORDER = (0, 7, 8, 1, 9, 10, 11, 12, 2, 6, 13, 3, 4, 14, 5)


    frame_rows = xs.at[t // 4, pl.ds(pl.multiple_of(lax.rem(t, 4) * PIECE, PIECE), PIECE)]

    def frame_copy(v):
        return pltpu.make_async_remote_copy(
            frames.at[v],
            frame_rows,
            frame_send.at[v],
            x_recv.at[t],
            device_id={"section": 0, "tm": 2 * v + 1},
            device_id_type=MESH,
        )

    sends_frames = (k == 1) & (t // 4 == c)

    @pl.when(sends_frames)
    def _():
        for v in range(UTTS):
            frame_copy(v).start()

    LEAD = ((1, 9, 10, 11), (12, 2, 6, 13), (3, 4, 14, 5))
    MATE = ((0, 7, 8), (1, 9, 10), (11, 12, 2, 6, 13, 3, 4, 14, 5))

    def push_part(part, first):
        @pl.when(first & (c == 0))
        def _():
            for i in LEAD[part]:
                push(i).start()

        @pl.when(first & (c == 1))
        def _():
            for i in MATE[part]:
                push(i).start()

    @pl.when(active)
    def _():
        for i in ORDER:
            local(i).start()
        push_part(0, k == 0)

        @pl.when(k > 0)
        def _():
            for i in ORDER:
                push(i).start()

    def piece_rows(j):
        return pl.ds(j * PIECE, PIECE)

    def forward(j):
        return pltpu.make_async_remote_copy(
            xs.at[2, piece_rows(j)],
            xs.at[0, piece_rows(j)],
            x_send.at[j],
            x_recv.at[j],
            device_id={"section": lax.rem(s + 2, 16), "tm": 2 * u + 1 - side},
            device_id_type=MESH,
        )

    def relayed(src, dst, send, recv, section, tm):
        return pltpu.make_async_remote_copy(
            src, dst, send, recv, device_id={"section": lax.rem(section + 16, 16), "tm": tm}, device_id_type=MESH
        )

    even = lax.rem(k, 2) == 0
    first_piece = xs.at[0, pl.ds(0, PIECE)]
    last_first = xs.at[2, pl.ds(0, PIECE)]

    def leave_z():
        return relayed(last_first, via_z, x_send.at[0], via_recv, s + 4, 2 * u + 1)

    def land_z():
        return relayed(via_z, first_piece, via_send, x_recv.at[0], s - 2, 2 * u + 1)

    idle = jnp.logical_not(active)

    @pl.when(idle & jnp.logical_not(even) & (k >= 3))
    def _():
        leave_z().wait_recv()
        land_z().start()
        land_z().wait_send()

    def scatter(slot, j):
        return pltpu.make_async_remote_copy(
            xs.at[slot + 1, piece_rows(j)],
            out.at[0, u],
            out_send.at[slot, j],
            out_recv.at[u],
            device_id={"section": 2 * k + slot, "tm": 4 * c + j},
            device_id_type=MESH,
        )

    def scatter_local(slot, j):
        return pltpu.make_async_copy(xs.at[slot + 1, piece_rows(j)], out.at[0, u], out_recv.at[u])

    def own_piece(slot, j):
        return (slot == c) & (4 * c + j == t)

    def emit(slot, j):
        @pl.when(own_piece(slot, j))
        def _():
            scatter_local(slot, j).start()

        @pl.when(jnp.logical_not(own_piece(slot, j)))
        def _():
            scatter(slot, j).start()

    own = pl.ds(pl.multiple_of(c * ROWS, ROWS), ROWS)

    def kv_part(slot, i, rows):
        ref = kv.at[slot, i // 2, rows, pl.ds((i % 2) * 512, 512)]
        return pltpu.make_async_remote_copy(
            ref, ref, kv_send.at[slot, i], kv_recv.at[slot, i], device_id=partner, device_id_type=MESH
        )

    def kv_copy(slot, i):
        return kv_part(slot, i, own)

    def kv_arrival(slot, i):
        return kv_part(slot, i, pl.ds(pl.multiple_of((1 - c) * ROWS, ROWS), ROWS))

    def hand_over():
        return pltpu.make_async_remote_copy(
            depth, res, hand_send, hand_recv, device_id=partner, device_id_type=MESH
        )

    def rim_copy(slot):
        return pltpu.make_async_remote_copy(
            rim_out.at[slot],
            rim_in.at[slot],
            rim_send.at[slot],
            rim_recv.at[slot],
            device_id=partner,
            device_id_type=MESH,
        )

    def run_slot(slot, carry, fast):
        mine = slot == c

        def wait_for(*ids):
            for i in ids:

                @pl.when(mine)
                def _(i=i):
                    local(i).wait()

                @pl.when(jnp.logical_not(mine))
                def _(i=i):
                    pull(i, slot).wait_recv()

        if fast:
            wait_for(*range(15))

        def ready(*ids):
            if not fast:
                wait_for(*ids)

        length = lengths[u]

        def input_ready(j):
            pltpu.make_async_remote_copy(
                first_piece, first_piece, x_send.at[0], x_recv.at[j], device_id=partner, device_id_type=MESH
            ).wait_recv()

        opening = (k == 0) & (slot == 0)
        passes = jnp.where(opening, jnp.where(c == 0, 4, 0), 2)

        def when_opening(condition):
            return pl.when(opening & condition) if not fast else (lambda f: None)

        if not fast:

            @pl.when(jnp.logical_not(opening & (c == 1)))
            def _():
                ready(0, 7, 8)

        def feed_forward(i, carry):
            group = i // 2
            source = xs.at[slot + group]
            rows = pl.ds(i * HALF, HALF) if fast else pl.ds(pl.multiple_of(lax.rem(i, 2) * HALF, HALF), HALF)

            @pl.when(slot == 0)
            def _():
                input_ready(2 * i)
                input_ready(2 * i + 1)

            act[rows] = normed(source[rows].astype(F32), vec[slot, 0]).astype(BF16)
            for n in range(4):
                cols = pl.ds(n * 512, 512)
                v = dot(act[rows], w_up[slot, :, cols])
                wide[rows, cols] = (v * sigmoid(v)).astype(BF16)
            for n in range(2):
                cols = pl.ds(n * 512, 512)
                v = dot(wide[rows], w_down[slot, :, cols])
                sums[group, rows, cols] = source[rows, cols].astype(F32) + 0.5 * v
            return carry

        if fast:
            for i in range(2):
                feed_forward(i, 0)
        else:
            lax.fori_loop(0, passes, feed_forward, 0)

        @when_opening(c == 0)
        def _():
            hand_over().start()

        @when_opening(c == 1)
        def _():
            hand_over().wait_recv()

        ready(1, 9, 10)
        act[...] = normed(res[...], vec[slot, 1]).astype(BF16)
        for i in range(4):
            cols = pl.ds((i // 2) * 512, 512)
            w = (w_key, w_value)[i % 2]
            kv[slot, i % 2, own, cols] = dot(act[...], w[slot, :, cols]).astype(BF16)
            kv_copy(slot, 2 * (i % 2) + i // 2).start()
        if not fast:
            push_part(1, opening)

        @pl.when(slot == 1)
        def _():
            for j in range(PIECES):
                emit(0, j)

        ready(11)
        for n in range(2):
            cols = pl.ds(n * 512, 512)
            wide[:, cols] = (dot(act[...], w_query[slot, :, cols]) * QUERY_SCALE).astype(BF16)
        kv_arrival(slot, 0).wait_recv()
        kv_arrival(slot, 2).wait_recv()

        low = lax.broadcasted_iota(jnp.int32, (ROWS, 128), 1) < 64
        one = jnp.where(lax.broadcasted_iota(jnp.int32, (ROWS, 128), 1) == 0, 1.0, 0.0).astype(BF16)
        ones = jnp.ones((LEN, 128), BF16)

        def pair_scores(g):
            cols = pl.ds(g * 128, 128)
            q = wide[:, cols]
            none = jnp.zeros_like(q)
            stacked = jnp.concatenate(
                [
                    jnp.concatenate([jnp.where(low, q, none), one], axis=1),
                    jnp.concatenate([jnp.where(low, none, q), one], axis=1),
                ],
                axis=0,
            )
            keys = jnp.concatenate([kv[slot, 0, :, cols], bias[...]], axis=1)
            return lax.dot_general(
                stacked, keys, (((1,), (1,)), ((), ())), preferred_element_type=F32
            )

        def pair_context(g, scores):
            cols = pl.ds(g * 128, 128)
            peak = jnp.max(scores, axis=-1, keepdims=True)
            weights = jnp.exp2(scores - peak).astype(BF16)
            values = jnp.concatenate([kv[slot, 1, :, cols], ones], axis=1)
            mixed = dot(weights, values)
            total = jnp.where(low, mixed[:ROWS, 128:], mixed[ROWS:, 128:])
            mixed = jnp.where(low, mixed[:ROWS, :128], mixed[ROWS:, :128])
            act[:, cols] = (mixed / total).astype(BF16)

        scores = pair_scores(0)
        for g in range(HEADS // 2):
            if g == 3:
                kv_arrival(slot, 1).wait_recv()
                kv_arrival(slot, 3).wait_recv()
            later = pair_scores(g + 1) if g + 1 < HEADS // 2 else None
            pair_context(g, scores)
            scores = later
        ready(12)

        def out_tile(n):
            cols = pl.ds(n * 512, 512)
            res[:, cols] = res[:, cols] + dot(act[...], w_out[slot, :, cols])

        for n in range(2):
            out_tile(n)
        ready(2, 13, 6)

        @when_opening(c == 0)
        def _():
            hand_over().wait_send()

        wide[:, :D] = normed(res[...], vec[slot, 2]).astype(BF16)
        row = c * ROWS + lax.broadcasted_iota(jnp.int32, (ROWS, 256), 0)
        keep = (row < length).astype(F32)

        def glu_tile(n):
            value = dot(wide[:, :D], w_expand[slot, :, pl.ds(n * 256, 256)])
            gate = dot(wide[:, :D], w_expand[slot, :, pl.ds(n * 256 + D, 256)])
            glu = (value * sigmoid(gate) * keep).astype(BF16)
            rim_out[slot, :, pl.ds(n * 256, 256)] = jnp.where(c == 0, glu[ROWS - 16 :], glu[:16])
            glu = glu.astype(F32)
            padded[2 * n, pl.ds(16, ROWS), :] = glu[:, :128]
            padded[2 * n + 1, pl.ds(16, ROWS), :] = glu[:, 128:]

        def conv_rows(n, base, blocks):
            cols = pl.ds(n * 128, 128)
            weights = [taps[slot, j, :, cols] for j in range(TAPS)]
            total = [None] * blocks
            for o in range(1, 8 * (blocks - 1) + TAPS + 1):
                v = padded[n, pl.ds(base + o, 8), :]
                for b in range(blocks):
                    j = o - 1 - 8 * b
                    if 0 <= j < TAPS:
                        term = v * weights[j]
                        total[b] = term if total[b] is None else total[b] + term
            for b in range(blocks):
                depth[pl.ds(base + 8 * b, 8), cols] = total[b]

        for n in range(5):
            if n < 4:
                glu_tile(n)
            if n == 3:
                rim_copy(slot).start()
                if not fast:
                    push_part(2, opening)
            if n > 0:
                for i in (2 * n - 2, 2 * n - 1):
                    conv_rows(i, 0, 16)
                    conv_rows(i, 128, 16)
        ready(3, 4)
        rim_copy(slot).wait_recv()
        inner_rim = pl.ds(pl.multiple_of((1 - c) * (ROWS + 16), 16), 16)
        edge = pl.multiple_of((1 - c) * (ROWS - 16), 16)
        for n in range(8):
            padded[n, inner_rim, :] = rim_in[slot, :, n * 128 : (n + 1) * 128].astype(F32)
            conv_rows(n, edge, 2)
        ready(14, 5)
        for h in range(2):
            rows = pl.ds(h * HALF, HALF)
            shifted = normed(depth[rows], vec[slot, 3]) + vec[slot, 4]
            act[rows] = (shifted * sigmoid(shifted)).astype(BF16)
            closing = res[rows] + dot(act[rows], w_shrink[slot])
            xs[slot + 1, rows] = normed(closing, vec[slot, 5]).astype(BF16)
            for j in (2 * h, 2 * h + 1):

                @pl.when((slot == 1) & (k < STAGES - 1))
                def _(j=j):
                    if j == 0:

                        @pl.when(even)
                        def _():
                            forward(0).start()

                        @pl.when(jnp.logical_not(even))
                        def _():
                            leave_z().start()

                    else:
                        forward(j).start()

                @pl.when((slot == 1) & (k == STAGES - 1))
                def _(j=j):
                    emit(1, j)

        @pl.when((slot == 1) & (k < STAGES - 1))
        def _():
            for j in range(PIECES):
                emit(1, j)

        return carry

    @pl.when(active)
    def _():
        seen = lax.broadcasted_iota(jnp.int32, (LEN, 128), 0) < lengths[u]
        bias[...] = jnp.where(seen, 0.0, -1e30).astype(BF16)
        for n in range(8):
            padded[n, pl.ds(0, 16), :] = jnp.zeros((16, 128), F32)
            padded[n, pl.ds(16 + ROWS, 16), :] = jnp.zeros((16, 128), F32)

        @pl.when(k == 0)
        def _():
            lax.fori_loop(0, 2, functools.partial(run_slot, fast=False), 0)

        @pl.when(k > 0)
        def _():
            lax.fori_loop(0, 2, functools.partial(run_slot, fast=True), 0)

        for i in ORDER:

            @pl.when(pushed(i))
            def _(i=i):
                push(i).wait_send()

        for slot in range(2):
            for i in range(4):
                kv_copy(slot, i).wait_send()
            rim_copy(slot).wait_send()
            for j in range(PIECES):

                @pl.when(jnp.logical_not(own_piece(slot, j)))
                def _(slot=slot, j=j):
                    scatter(slot, j).wait_send()

        @pl.when(k < STAGES - 1)
        def _():
            for j in range(PIECES):
                forward(j).wait_send()

    @pl.when(sends_frames)
    def _():
        for v in range(UTTS):
            frame_copy(v).wait_send()

    for v in range(UTTS):
        itself = (t == 2 * v + side) & (c == t // 4)
        landed = out.at[0, v]

        @pl.when(itself)
        def _(v=v, landed=landed):
            pltpu.make_async_copy(xs.at[0, piece_rows(0)], landed, out_recv.at[v]).wait()

        @pl.when(jnp.logical_not(itself))
        def _(v=v, landed=landed):
            pltpu.make_async_remote_copy(
                landed, landed, out_send.at[0, 0], out_recv.at[v], device_id=partner, device_id_type=MESH
            ).wait_recv()


def body(
    frames,
    lengths,
    ffn_gain,
    ffn_up,
    ffn_down,
    attn_gain,
    query_weight,
    key_weight,
    value_weight,
    out_weight,
    conv_gain,
    expand_weight,
    depth_weight,
    depth_gain,
    norm_shift,
    shrink_weight,
    final_gain,
):
    anywhere = pl.BlockSpec(memory_space=pl.ANY)
    dma = pltpu.SemaphoreType.DMA
    return pl.pallas_call(
        block_kernel,
        name="conformer",
        out_shape=jax.ShapeDtypeStruct((1, UTTS, PIECE, D), BF16),
        in_specs=[pl.BlockSpec(memory_space=pltpu.SMEM)] + [anywhere] * 16,
        out_specs=anywhere,
        scratch_shapes=[pltpu.VMEM((2,) + shape, BF16) for shape in SHAPES]
        + [
            pltpu.VMEM((2, 6, 1, D), F32),
            pltpu.VMEM((2, TAPS, 1, D), F32),
            pltpu.VMEM((3, ROWS, D), BF16),
            pltpu.VMEM((ROWS, D), BF16),
            pltpu.VMEM((ROWS, FF), BF16),
            pltpu.VMEM((2, ROWS, D), F32),
            pltpu.VMEM((2, 2, LEN, D), BF16),
            pltpu.VMEM((2, 16, D), BF16),
            pltpu.VMEM((2, 16, D), BF16),
            pltpu.VMEM((LEN, 128), BF16),
            pltpu.VMEM((8, ROWS + 32, 128), F32),
            pltpu.VMEM((PIECE, D), BF16),
            dma((15,)),
            dma((15,)),
            dma((15,)),
            dma((PIECES,)),
            dma((2 * PIECES,)),
            dma((2, PIECES)),
            dma((UTTS,)),
            dma((2, 4)),
            dma((2, 4)),
            dma((2,)),
            dma((2,)),
            dma((UTTS,)),
            dma,
            dma,
            dma,
            dma,
        ],
        compiler_params=pltpu.CompilerParams(
            has_side_effects=True, vmem_limit_bytes=67043328
        ),
    )(
        lengths,
        frames,
        ffn_gain,
        attn_gain,
        conv_gain,
        depth_gain,
        norm_shift,
        final_gain,
        jnp.transpose(depth_weight, (1, 0, 2)),
        ffn_up,
        ffn_down,
        key_weight,
        value_weight,
        query_weight,
        out_weight,
        expand_weight,
        shrink_weight,
    )


def solution(mesh):
    return jax.shard_map(
        body,
        mesh=mesh,
        in_specs=(
            P(None, "tm", None),
            P(),
            P("section", None),
            P("section", None, None),
            P("section", None, None),
            P("section", None),
            P("section", None, None),
            P("section", None, None),
            P("section", None, None),
            P("section", None, None),
            P("section", None),
            P("section", None, None),
            P("section", None, None),
            P("section", None),
            P("section", None),
            P("section", None, None),
            P("section", None),
        ),
        out_specs=P("section", None, "tm", None),
        check_vma=False,
    )
```

```python
import functools

import jax
import jax.numpy as jnp
from jax import lax
from jax.experimental import pallas as pl
from jax.experimental.pallas import tpu as pltpu
from jax.sharding import PartitionSpec as P

MESH = pl.DeviceIdType.MESH
F32 = jnp.float32
BF16 = jnp.bfloat16
EPS = 1e-05
D = 1024
FF = 2048
HEADS = 16
ROWS = 256
LEN = 512
TAPS = 31
UTTS = 4
STAGES = 8
PIECE = 64
PIECES = ROWS // PIECE
HALF = ROWS // 2
CHUNK = 16
QUERY_SCALE = 0.125 * 1.4426950408889634
SHAPES = ((D, FF), (FF, D), (D, D), (D, D), (D, D), (D, D), (D, 2 * D), (D, D))


def sigmoid(v):
    return 0.5 * jnp.tanh(0.5 * v) + 0.5


def normed(v, gain):
    mean = jnp.mean(v, axis=-1, keepdims=True)
    centred = v - mean
    spread = jnp.mean(centred * centred, axis=-1, keepdims=True)
    return centred * lax.rsqrt(spread + EPS) * gain


def dot(a, b):
    return jnp.dot(a, b, preferred_element_type=F32)


def block_kernel(
    lengths,
    frames,
    ffn_gain,
    attn_gain,
    conv_gain,
    depth_gain,
    norm_shift,
    final_gain,
    depth_weight,
    h_up,
    h_down,
    h_key,
    h_value,
    h_query,
    h_out,
    h_expand,
    h_shrink,
    out,
    w_up,
    w_down,
    w_key,
    w_value,
    w_query,
    w_out,
    w_expand,
    w_shrink,
    vec,
    taps,
    xs,
    act,
    wide,
    sums,
    kv,
    rim_out,
    rim_in,
    bias,
    padded,
    via_x,
    via_z,
    local_sem,
    push_sem,
    pull_sem,
    x_send,
    x_recv,
    out_send,
    out_recv,
    kv_send,
    kv_recv,
    rim_send,
    rim_recv,
    frame_send,
    via_send,
    via_recv,
    chunk_send,
    chunk_recv,
    hand_send,
    hand_recv,
):
    res, depth = sums.at[0], sums.at[1]
    s = lax.axis_index("section")
    t = lax.axis_index("tm")
    k = s // 2
    c = lax.rem(s, 2)
    u = t // 2
    side = 1 - lax.rem(k, 2)
    active = lax.rem(t, 2) == side
    partner = {"section": 2 * k + 1 - c, "tm": t}
    here = {"section": s, "tm": t}
    del here

    hbm = (h_up, h_down, h_key, h_value, h_query, h_out, h_expand, h_shrink)
    vmem = (w_up, w_down, w_key, w_value, w_query, w_out, w_expand, w_shrink)
    small = (ffn_gain, attn_gain, conv_gain, depth_gain, norm_shift, final_gain)

    def sources():
        pairs = [(small[i], vec.at[c, i]) for i in range(6)]
        pairs += [(depth_weight, taps.at[c])]
        pairs += [(hbm[i].at[0], vmem[i].at[c]) for i in range(8)]
        return pairs

    def arrivals(slot):
        refs = [vec.at[slot, i] for i in range(6)] + [taps.at[slot]]
        return refs + [vmem[i].at[slot] for i in range(8)]

    def local(i):
        src, dst = sources()[i]
        return pltpu.make_async_copy(src, dst, local_sem.at[i])

    def push(i):
        src, dst = sources()[i]
        return pltpu.make_async_remote_copy(
            src, dst, push_sem.at[i], pull_sem.at[i], device_id=partner, device_id_type=MESH
        )

    def pull(i, slot):
        ref = arrivals(slot)[i]
        return pltpu.make_async_remote_copy(
            ref, ref, push_sem.at[i], pull_sem.at[i], device_id=partner, device_id_type=MESH
        )

    lead = (k == 0) & (c == 0)

    def pushed(i):
        return jnp.logical_not(lead) if i in (0, 7, 8) else k >= 0

    ORDER = (0, 7, 8, 1, 9, 10, 11, 12, 2, 6, 13, 3, 4, 14, 5)


    frame_rows = xs.at[t // 4, pl.ds(pl.multiple_of(lax.rem(t, 4) * PIECE, PIECE), PIECE)]

    def frame_copy(v):
        return pltpu.make_async_remote_copy(
            frames.at[v],
            frame_rows,
            frame_send.at[v],
            x_recv.at[t],
            device_id={"section": 0, "tm": 2 * v + 1},
            device_id_type=MESH,
        )

    def frame_local(v):
        return pltpu.make_async_copy(frames.at[v], frame_rows, x_recv.at[t])

    sends_frames = (k == 0) & (t // 4 == c)
    for v in range(UTTS):
        to_itself = (c == 0) & (t == 2 * v + 1)

        @pl.when(sends_frames & jnp.logical_not(to_itself))
        def _(v=v):
            frame_copy(v).start()

        @pl.when(sends_frames & to_itself)
        def _(v=v):
            frame_local(v).start()

    LEAD = ((1, 9, 10, 11), (12, 2, 6, 13), (3, 4, 14, 5))
    MATE = ((0, 7, 8), (1, 9, 10), (11, 12, 2, 6, 13, 3, 4, 14, 5))

    def push_part(part, first):
        @pl.when(first & (c == 0))
        def _():
            for i in LEAD[part]:
                push(i).start()

        @pl.when(first & (c == 1))
        def _():
            for i in MATE[part]:
                push(i).start()

    @pl.when(active)
    def _():
        for i in ORDER:
            local(i).start()
        push_part(0, k == 0)

        @pl.when(k > 0)
        def _():
            for i in ORDER:
                push(i).start()

    def piece_rows(j):
        return pl.ds(j * PIECE, PIECE)

    def forward(j):
        return pltpu.make_async_remote_copy(
            xs.at[2, piece_rows(j)],
            xs.at[0, piece_rows(j)],
            x_send.at[j],
            x_recv.at[j],
            device_id={"section": lax.rem(s + 2, 16), "tm": 2 * u + 1 - side},
            device_id_type=MESH,
        )

    def relayed(src, dst, send, recv, section, tm):
        return pltpu.make_async_remote_copy(
            src, dst, send, recv, device_id={"section": lax.rem(section + 16, 16), "tm": tm}, device_id_type=MESH
        )

    even = lax.rem(k, 2) == 0
    first_piece = xs.at[0, pl.ds(0, PIECE)]
    last_first = xs.at[2, pl.ds(0, PIECE)]

    def chunk(ref, n):
        return ref.at[pl.ds(n * CHUNK, CHUNK)]

    def leave_x(n):
        return relayed(
            chunk(xs.at[2], n), chunk(via_x, n), x_send.at[0], chunk_recv.at[n], s, 2 * u
        )

    def pass_x(n):
        return relayed(
            chunk(via_x, n), chunk(via_x, n), chunk_send.at[n], chunk_recv.at[n], s + 2, 2 * u + 1
        )

    def land_x(n):
        return relayed(
            chunk(via_x, n), chunk(xs.at[0], n), chunk_send.at[n], x_recv.at[0], s, 2 * u
        )

    def leave_z():
        return relayed(last_first, via_z, x_send.at[0], via_recv, s + 4, 2 * u + 1)

    def land_z():
        return relayed(via_z, first_piece, via_send, x_recv.at[0], s - 2, 2 * u + 1)

    idle = jnp.logical_not(active)

    @pl.when(idle & even)
    def _():
        for n in range(PIECE // CHUNK):
            pass_x(n).wait_recv()
            pass_x(n).start()
        for n in range(PIECE // CHUNK):
            pass_x(n).wait_send()

    @pl.when(idle & jnp.logical_not(even))
    def _():
        @pl.when(k >= 3)
        def _():
            leave_z().wait_recv()
            land_z().start()
            land_z().wait_send()

        for n in range(PIECE // CHUNK):
            pass_x(n).wait_recv()
            land_x(n).start()
        for n in range(PIECE // CHUNK):
            land_x(n).wait_send()

    def scatter(slot, j):
        return pltpu.make_async_remote_copy(
            xs.at[slot + 1, piece_rows(j)],
            out.at[0, u],
            out_send.at[slot, j],
            out_recv.at[u],
            device_id={"section": 2 * k + slot, "tm": 4 * c + j},
            device_id_type=MESH,
        )

    def scatter_local(slot, j):
        return pltpu.make_async_copy(xs.at[slot + 1, piece_rows(j)], out.at[0, u], out_recv.at[u])

    def own_piece(slot, j):
        return (slot == c) & (4 * c + j == t)

    def emit(slot, j):
        @pl.when(own_piece(slot, j))
        def _():
            scatter_local(slot, j).start()

        @pl.when(jnp.logical_not(own_piece(slot, j)))
        def _():
            scatter(slot, j).start()

    own = pl.ds(pl.multiple_of(c * ROWS, ROWS), ROWS)

    def kv_part(slot, i, rows):
        ref = kv.at[slot, i // 2, rows, pl.ds((i % 2) * 512, 512)]
        return pltpu.make_async_remote_copy(
            ref, ref, kv_send.at[slot, i], kv_recv.at[slot, i], device_id=partner, device_id_type=MESH
        )

    def kv_copy(slot, i):
        return kv_part(slot, i, own)

    def kv_arrival(slot, i):
        return kv_part(slot, i, pl.ds(pl.multiple_of((1 - c) * ROWS, ROWS), ROWS))

    def hand_over():
        return pltpu.make_async_remote_copy(
            depth, res, hand_send, hand_recv, device_id=partner, device_id_type=MESH
        )

    def rim_copy(slot):
        return pltpu.make_async_remote_copy(
            rim_out.at[slot],
            rim_in.at[slot],
            rim_send.at[slot],
            rim_recv.at[slot],
            device_id=partner,
            device_id_type=MESH,
        )

    def run_slot(slot, carry, fast):
        mine = slot == c

        def wait_for(*ids):
            for i in ids:

                @pl.when(mine)
                def _(i=i):
                    local(i).wait()

                @pl.when(jnp.logical_not(mine))
                def _(i=i):
                    pull(i, slot).wait_recv()

        if fast:
            wait_for(*range(15))

        def ready(*ids):
            if not fast:
                wait_for(*ids)

        length = lengths[u]

        def input_ready(j):
            def remote():
                pltpu.make_async_remote_copy(
                    first_piece, first_piece, x_send.at[0], x_recv.at[j], device_id=partner, device_id_type=MESH
                ).wait_recv()

            if fast:
                remote()
                return
            itself = lead & (j == t) & (t < 4)

            @pl.when(itself)
            def _():
                frame_local(u).wait()

            pl.when(jnp.logical_not(itself))(remote)

        opening = (k == 0) & (slot == 0)
        passes = jnp.where(opening, jnp.where(c == 0, 4, 0), 2)

        def when_opening(condition):
            return pl.when(opening & condition) if not fast else (lambda f: None)

        if not fast:

            @pl.when(jnp.logical_not(opening & (c == 1)))
            def _():
                ready(0, 7, 8)

        def feed_forward(i, carry):
            group = i // 2
            source = xs.at[slot + group]
            rows = pl.ds(i * HALF, HALF) if fast else pl.ds(pl.multiple_of(lax.rem(i, 2) * HALF, HALF), HALF)

            @pl.when(slot == 0)
            def _():
                input_ready(2 * i)
                input_ready(2 * i + 1)

            act[rows] = normed(source[rows].astype(F32), vec[slot, 0]).astype(BF16)
            for n in range(4):
                cols = pl.ds(n * 512, 512)
                v = dot(act[rows], w_up[slot, :, cols])
                wide[rows, cols] = (v * sigmoid(v)).astype(BF16)
            for n in range(2):
                cols = pl.ds(n * 512, 512)
                v = dot(wide[rows], w_down[slot, :, cols])
                sums[group, rows, cols] = source[rows, cols].astype(F32) + 0.5 * v
            return carry

        if not fast:
            lax.fori_loop(0, passes, feed_forward, 0)

        @when_opening(c == 0)
        def _():
            hand_over().start()

        @when_opening(c == 1)
        def _():
            hand_over().wait_recv()

        ready(1, 9, 10)

        def attention_input(rows, offset, length, share):
            act[rows] = normed(res[rows], vec[slot, 1]).astype(BF16)
            mine_rows = pl.ds(pl.multiple_of(c * ROWS + offset, HALF), length)
            for i in range(4):
                cols = pl.ds((i // 2) * 512, 512)
                w = (w_key, w_value)[i % 2]
                kv[slot, i % 2, mine_rows, cols] = dot(act[rows], w[slot, :, cols]).astype(BF16)
                if share:
                    kv_copy(slot, 2 * (i % 2) + i // 2).start()

        if fast:
            for i in range(2):
                feed_forward(i, 0)
                attention_input(pl.ds(i * HALF, HALF), i * HALF, HALF, i == 1)
        else:
            attention_input(pl.ds(0, ROWS), 0, ROWS, True)
        if not fast:
            push_part(1, opening)

        @pl.when(slot == 1)
        def _():
            for j in range(PIECES):
                emit(0, j)

        ready(11)
        for n in range(2):
            cols = pl.ds(n * 512, 512)
            wide[:, cols] = (dot(act[...], w_query[slot, :, cols]) * QUERY_SCALE).astype(BF16)
        kv_arrival(slot, 0).wait_recv()
        kv_arrival(slot, 2).wait_recv()

        low = lax.broadcasted_iota(jnp.int32, (ROWS, 128), 1) < 64
        one = jnp.where(lax.broadcasted_iota(jnp.int32, (ROWS, 128), 1) == 0, 1.0, 0.0).astype(BF16)
        ones = jnp.ones((LEN, 128), BF16)

        def pair_scores(g):
            cols = pl.ds(g * 128, 128)
            q = wide[:, cols]
            none = jnp.zeros_like(q)
            stacked = jnp.concatenate(
                [
                    jnp.concatenate([jnp.where(low, q, none), one], axis=1),
                    jnp.concatenate([jnp.where(low, none, q), one], axis=1),
                ],
                axis=0,
            )
            keys = jnp.concatenate([kv[slot, 0, :, cols], bias[...]], axis=1)
            return lax.dot_general(
                stacked, keys, (((1,), (1,)), ((), ())), preferred_element_type=F32
            )

        def pair_context(g, scores):
            cols = pl.ds(g * 128, 128)
            peak = jnp.max(scores, axis=-1, keepdims=True)
            weights = jnp.exp2(scores - peak).astype(BF16)
            values = jnp.concatenate([kv[slot, 1, :, cols], ones], axis=1)
            mixed = dot(weights, values)
            total = jnp.where(low, mixed[:ROWS, 128:], mixed[ROWS:, 128:])
            mixed = jnp.where(low, mixed[:ROWS, :128], mixed[ROWS:, :128])
            act[:, cols] = (mixed / total).astype(BF16)

        scores = pair_scores(0)
        for g in range(HEADS // 2):
            if g == 3:
                kv_arrival(slot, 1).wait_recv()
                kv_arrival(slot, 3).wait_recv()
            later = pair_scores(g + 1) if g + 1 < HEADS // 2 else None
            pair_context(g, scores)
            scores = later
        ready(12)

        def out_tile(n):
            cols = pl.ds(n * 512, 512)
            res[:, cols] = res[:, cols] + dot(act[...], w_out[slot, :, cols])

        for n in range(2):
            out_tile(n)
        ready(2, 13, 6)

        @when_opening(c == 0)
        def _():
            hand_over().wait_send()

        wide[:, :D] = normed(res[...], vec[slot, 2]).astype(BF16)
        row = c * ROWS + lax.broadcasted_iota(jnp.int32, (ROWS, 256), 0)
        keep = (row < length).astype(F32)

        def glu_tile(n):
            value = dot(wide[:, :D], w_expand[slot, :, pl.ds(n * 256, 256)])
            gate = dot(wide[:, :D], w_expand[slot, :, pl.ds(n * 256 + D, 256)])
            glu = (value * sigmoid(gate) * keep).astype(BF16)
            rim_out[slot, :, pl.ds(n * 256, 256)] = jnp.where(c == 0, glu[ROWS - 16 :], glu[:16])
            glu = glu.astype(F32)
            padded[2 * n, pl.ds(16, ROWS), :] = glu[:, :128]
            padded[2 * n + 1, pl.ds(16, ROWS), :] = glu[:, 128:]

        def conv_rows(n, base, blocks):
            cols = pl.ds(n * 128, 128)
            weights = [taps[slot, j, :, cols] for j in range(TAPS)]
            total = [None] * blocks
            for o in range(1, 8 * (blocks - 1) + TAPS + 1):
                v = padded[n, pl.ds(base + o, 8), :]
                for b in range(blocks):
                    j = o - 1 - 8 * b
                    if 0 <= j < TAPS:
                        term = v * weights[j]
                        total[b] = term if total[b] is None else total[b] + term
            for b in range(blocks):
                depth[pl.ds(base + 8 * b, 8), cols] = total[b]

        for n in range(5):
            if n < 4:
                glu_tile(n)
            if n == 3:
                rim_copy(slot).start()
                if not fast:
                    push_part(2, opening)
            if n > 0:
                for i in (2 * n - 2, 2 * n - 1):
                    conv_rows(i, 0, 16)
                    conv_rows(i, 128, 16)
        ready(3, 4)
        rim_copy(slot).wait_recv()
        inner_rim = pl.ds(pl.multiple_of((1 - c) * (ROWS + 16), 16), 16)
        edge = pl.multiple_of((1 - c) * (ROWS - 16), 16)
        for n in range(8):
            padded[n, inner_rim, :] = rim_in[slot, :, n * 128 : (n + 1) * 128].astype(F32)
            conv_rows(n, edge, 2)
        ready(14, 5)
        for h in range(2):
            rows = pl.ds(h * HALF, HALF)
            shifted = normed(depth[rows], vec[slot, 3]) + vec[slot, 4]
            act[rows] = (shifted * sigmoid(shifted)).astype(BF16)
            closing = res[rows] + dot(act[rows], w_shrink[slot])
            xs[slot + 1, rows] = normed(closing, vec[slot, 5]).astype(BF16)
            for j in (2 * h, 2 * h + 1):

                @pl.when((slot == 1) & (k < STAGES - 1))
                def _(j=j):
                    if j == 0:

                        @pl.when(even)
                        def _():
                            for n in range(PIECE // CHUNK):
                                leave_x(n).start()

                        @pl.when(jnp.logical_not(even))
                        def _():
                            leave_z().start()

                    else:
                        forward(j).start()

                @pl.when((slot == 1) & (k == STAGES - 1))
                def _(j=j):
                    emit(1, j)

        @pl.when((slot == 1) & (k < STAGES - 1))
        def _():
            for j in range(PIECES):
                emit(1, j)

        return carry

    @pl.when(active)
    def _():
        seen = lax.broadcasted_iota(jnp.int32, (LEN, 128), 0) < lengths[u]
        bias[...] = jnp.where(seen, 0.0, -1e30).astype(BF16)
        for n in range(8):
            padded[n, pl.ds(0, 16), :] = jnp.zeros((16, 128), F32)
            padded[n, pl.ds(16 + ROWS, 16), :] = jnp.zeros((16, 128), F32)

        @pl.when(k == 0)
        def _():
            lax.fori_loop(0, 2, functools.partial(run_slot, fast=False), 0)

        @pl.when(k > 0)
        def _():
            lax.fori_loop(0, 2, functools.partial(run_slot, fast=True), 0)

        for i in ORDER:

            @pl.when(pushed(i))
            def _(i=i):
                push(i).wait_send()

        for slot in range(2):
            for i in range(4):
                kv_copy(slot, i).wait_send()
            rim_copy(slot).wait_send()
            for j in range(PIECES):

                @pl.when(jnp.logical_not(own_piece(slot, j)))
                def _(slot=slot, j=j):
                    scatter(slot, j).wait_send()

        @pl.when(k < STAGES - 1)
        def _():
            for j in range(PIECES):
                forward(j).wait_send()

    for v in range(UTTS):

        @pl.when(sends_frames & jnp.logical_not((c == 0) & (t == 2 * v + 1)))
        def _(v=v):
            frame_copy(v).wait_send()

    for v in range(UTTS):
        itself = (t == 2 * v + side) & (c == t // 4)
        landed = out.at[0, v]

        @pl.when(itself)
        def _(v=v, landed=landed):
            pltpu.make_async_copy(xs.at[0, piece_rows(0)], landed, out_recv.at[v]).wait()

        @pl.when(jnp.logical_not(itself))
        def _(v=v, landed=landed):
            pltpu.make_async_remote_copy(
                landed, landed, out_send.at[0, 0], out_recv.at[v], device_id=partner, device_id_type=MESH
            ).wait_recv()


def body(
    frames,
    lengths,
    ffn_gain,
    ffn_up,
    ffn_down,
    attn_gain,
    query_weight,
    key_weight,
    value_weight,
    out_weight,
    conv_gain,
    expand_weight,
    depth_weight,
    depth_gain,
    norm_shift,
    shrink_weight,
    final_gain,
):
    anywhere = pl.BlockSpec(memory_space=pl.ANY)
    dma = pltpu.SemaphoreType.DMA
    return pl.pallas_call(
        block_kernel,
        name="conformer",
        out_shape=jax.ShapeDtypeStruct((1, UTTS, PIECE, D), BF16),
        in_specs=[pl.BlockSpec(memory_space=pltpu.SMEM)] + [anywhere] * 16,
        out_specs=anywhere,
        scratch_shapes=[pltpu.VMEM((2,) + shape, BF16) for shape in SHAPES]
        + [
            pltpu.VMEM((2, 6, 1, D), F32),
            pltpu.VMEM((2, TAPS, 1, D), F32),
            pltpu.VMEM((3, ROWS, D), BF16),
            pltpu.VMEM((ROWS, D), BF16),
            pltpu.VMEM((ROWS, FF), BF16),
            pltpu.VMEM((2, ROWS, D), F32),
            pltpu.VMEM((2, 2, LEN, D), BF16),
            pltpu.VMEM((2, 16, D), BF16),
            pltpu.VMEM((2, 16, D), BF16),
            pltpu.VMEM((LEN, 128), BF16),
            pltpu.VMEM((8, ROWS + 32, 128), F32),
            pltpu.VMEM((PIECE, D), BF16),
            pltpu.VMEM((PIECE, D), BF16),
            dma((15,)),
            dma((15,)),
            dma((15,)),
            dma((PIECES,)),
            dma((2 * PIECES,)),
            dma((2, PIECES)),
            dma((UTTS,)),
            dma((2, 4)),
            dma((2, 4)),
            dma((2,)),
            dma((2,)),
            dma((UTTS,)),
            dma,
            dma,
            dma((PIECE // CHUNK,)),
            dma((PIECE // CHUNK,)),
            dma,
            dma,
        ],
        compiler_params=pltpu.CompilerParams(
            has_side_effects=True, vmem_limit_bytes=67043328
        ),
    )(
        lengths,
        frames,
        ffn_gain,
        attn_gain,
        conv_gain,
        depth_gain,
        norm_shift,
        final_gain,
        jnp.transpose(depth_weight, (1, 0, 2)),
        ffn_up,
        ffn_down,
        key_weight,
        value_weight,
        query_weight,
        out_weight,
        expand_weight,
        shrink_weight,
    )


def solution(mesh):
    return jax.shard_map(
        body,
        mesh=mesh,
        in_specs=(
            P(None, "tm", None),
            P(),
            P("section", None),
            P("section", None, None),
            P("section", None, None),
            P("section", None),
            P("section", None, None),
            P("section", None, None),
            P("section", None, None),
            P("section", None, None),
            P("section", None),
            P("section", None, None),
            P("section", None, None),
            P("section", None),
            P("section", None),
            P("section", None, None),
            P("section", None),
        ),
        out_specs=P("section", None, "tm", None),
        check_vma=False,
    )
```

```python
import functools

import jax
import jax.numpy as jnp
from jax import lax
from jax.experimental import pallas as pl
from jax.experimental.pallas import tpu as pltpu
from jax.sharding import PartitionSpec as P

MESH = pl.DeviceIdType.MESH
F32 = jnp.float32
BF16 = jnp.bfloat16
EPS = 1e-05
D = 1024
FF = 2048
HEADS = 16
ROWS = 256
LEN = 512
TAPS = 31
UTTS = 4
STAGES = 8
PIECE = 64
PIECES = ROWS // PIECE
HALF = ROWS // 2
CHUNK = 16
QUERY_SCALE = 0.125 * 1.4426950408889634
SHAPES = ((D, FF), (FF, D), (D, D), (D, D), (D, D), (D, D), (D, 2 * D), (D, D))


def sigmoid(v):
    return 0.5 * jnp.tanh(0.5 * v) + 0.5


def normed(v, gain):
    mean = jnp.mean(v, axis=-1, keepdims=True)
    centred = v - mean
    spread = jnp.mean(centred * centred, axis=-1, keepdims=True)
    return centred * lax.rsqrt(spread + EPS) * gain


def dot(a, b):
    return jnp.dot(a, b, preferred_element_type=F32)


def block_kernel(
    lengths,
    frames,
    ffn_gain,
    attn_gain,
    conv_gain,
    depth_gain,
    norm_shift,
    final_gain,
    depth_weight,
    h_up,
    h_down,
    h_key,
    h_value,
    h_query,
    h_out,
    h_expand,
    h_shrink,
    out,
    w_up,
    w_down,
    w_key,
    w_value,
    w_query,
    w_out,
    w_expand,
    w_shrink,
    vec,
    taps,
    xs,
    act,
    wide,
    sums,
    kv,
    rim_out,
    rim_in,
    bias,
    padded,
    via_x,
    via_z,
    local_sem,
    push_sem,
    pull_sem,
    x_send,
    x_recv,
    out_send,
    out_recv,
    kv_send,
    kv_recv,
    rim_send,
    rim_recv,
    frame_send,
    via_send,
    via_recv,
    chunk_send,
    chunk_recv,
    hand_send,
    hand_recv,
):
    res, depth = sums.at[0], sums.at[1]
    s = lax.axis_index("section")
    t = lax.axis_index("tm")
    k = s // 2
    c = lax.rem(s, 2)
    u = t // 2
    side = 1 - lax.rem(k, 2)
    active = lax.rem(t, 2) == side
    partner = {"section": 2 * k + 1 - c, "tm": t}
    here = {"section": s, "tm": t}
    del here

    hbm = (h_up, h_down, h_key, h_value, h_query, h_out, h_expand, h_shrink)
    vmem = (w_up, w_down, w_key, w_value, w_query, w_out, w_expand, w_shrink)
    small = (ffn_gain, attn_gain, conv_gain, depth_gain, norm_shift, final_gain)

    def sources():
        pairs = [(small[i], vec.at[c, i]) for i in range(6)]
        pairs += [(depth_weight, taps.at[c])]
        pairs += [(hbm[i].at[0], vmem[i].at[c]) for i in range(8)]
        return pairs

    def arrivals(slot):
        refs = [vec.at[slot, i] for i in range(6)] + [taps.at[slot]]
        return refs + [vmem[i].at[slot] for i in range(8)]

    def local(i):
        src, dst = sources()[i]
        return pltpu.make_async_copy(src, dst, local_sem.at[i])

    def push(i):
        src, dst = sources()[i]
        return pltpu.make_async_remote_copy(
            src, dst, push_sem.at[i], pull_sem.at[i], device_id=partner, device_id_type=MESH
        )

    def pull(i, slot):
        ref = arrivals(slot)[i]
        return pltpu.make_async_remote_copy(
            ref, ref, push_sem.at[i], pull_sem.at[i], device_id=partner, device_id_type=MESH
        )

    lead = (k == 0) & (c == 0)

    def pushed(i):
        return jnp.logical_not(lead) if i in (0, 7, 8) else k >= 0

    ORDER = (0, 7, 8, 1, 9, 10, 11, 12, 2, 6, 13, 3, 4, 14, 5)


    frame_rows = xs.at[t // 4, pl.ds(pl.multiple_of(lax.rem(t, 4) * PIECE, PIECE), PIECE)]

    def frame_copy(v):
        return pltpu.make_async_remote_copy(
            frames.at[v],
            frame_rows,
            frame_send.at[v],
            x_recv.at[t],
            device_id={"section": 0, "tm": 2 * v + 1},
            device_id_type=MESH,
        )

    def frame_local(v):
        return pltpu.make_async_copy(frames.at[v], frame_rows, x_recv.at[t])

    sends_frames = (k == 0) & (t // 4 == c)
    for v in range(UTTS):
        to_itself = (c == 0) & (t == 2 * v + 1)

        @pl.when(sends_frames & jnp.logical_not(to_itself))
        def _(v=v):
            frame_copy(v).start()

        @pl.when(sends_frames & to_itself)
        def _(v=v):
            frame_local(v).start()

    LEAD = ((1, 9, 10, 11), (12, 2, 6, 13), (3, 4, 14, 5))
    MATE = ((0, 7, 8), (1, 9, 10), (11, 12, 2, 6, 13, 3, 4, 14, 5))

    def push_part(part, first):
        @pl.when(first & (c == 0))
        def _():
            for i in LEAD[part]:
                push(i).start()

        @pl.when(first & (c == 1))
        def _():
            for i in MATE[part]:
                push(i).start()

    @pl.when(active)
    def _():
        for i in ORDER:
            local(i).start()
        push_part(0, k == 0)

        @pl.when(k > 0)
        def _():
            for i in ORDER:
                push(i).start()

    def piece_rows(j):
        return pl.ds(j * PIECE, PIECE)

    def forward(j):
        return pltpu.make_async_remote_copy(
            xs.at[2, piece_rows(j)],
            xs.at[0, piece_rows(j)],
            x_send.at[j],
            x_recv.at[j],
            device_id={"section": lax.rem(s + 2, 16), "tm": 2 * u + 1 - side},
            device_id_type=MESH,
        )

    def relayed(src, dst, send, recv, section, tm):
        return pltpu.make_async_remote_copy(
            src, dst, send, recv, device_id={"section": lax.rem(section + 16, 16), "tm": tm}, device_id_type=MESH
        )

    even = lax.rem(k, 2) == 0
    first_piece = xs.at[0, pl.ds(0, PIECE)]
    last_first = xs.at[2, pl.ds(0, PIECE)]

    def chunk(ref, n):
        return ref.at[pl.ds(n * CHUNK, CHUNK)]

    def leave_x(n):
        return relayed(
            chunk(xs.at[2], n), chunk(via_x, n), x_send.at[0], chunk_recv.at[n], s, 2 * u
        )

    def pass_x(n):
        return relayed(
            chunk(via_x, n), chunk(via_x, n), chunk_send.at[n], chunk_recv.at[n], s + 2, 2 * u + 1
        )

    def land_x(n):
        return relayed(
            chunk(via_x, n), chunk(xs.at[0], n), chunk_send.at[n], x_recv.at[0], s, 2 * u
        )

    def leave_z():
        return relayed(last_first, via_z, x_send.at[0], via_recv, s + 4, 2 * u + 1)

    def land_z():
        return relayed(via_z, first_piece, via_send, x_recv.at[0], s - 2, 2 * u + 1)

    idle = jnp.logical_not(active)

    @pl.when(idle & even)
    def _():
        for n in range(PIECE // CHUNK):
            pass_x(n).wait_recv()
            pass_x(n).start()
        for n in range(PIECE // CHUNK):
            pass_x(n).wait_send()

    @pl.when(idle & jnp.logical_not(even))
    def _():
        @pl.when(k >= 3)
        def _():
            leave_z().wait_recv()
            land_z().start()
            land_z().wait_send()

        for n in range(PIECE // CHUNK):
            pass_x(n).wait_recv()
            land_x(n).start()
        for n in range(PIECE // CHUNK):
            land_x(n).wait_send()

    def scatter(slot, j):
        return pltpu.make_async_remote_copy(
            xs.at[slot + 1, piece_rows(j)],
            out.at[0, u],
            out_send.at[slot, j],
            out_recv.at[u],
            device_id={"section": 2 * k + slot, "tm": 4 * c + j},
            device_id_type=MESH,
        )

    def scatter_local(slot, j):
        return pltpu.make_async_copy(xs.at[slot + 1, piece_rows(j)], out.at[0, u], out_recv.at[u])

    def own_piece(slot, j):
        return (slot == c) & (4 * c + j == t)

    def emit(slot, j):
        @pl.when(own_piece(slot, j))
        def _():
            scatter_local(slot, j).start()

        @pl.when(jnp.logical_not(own_piece(slot, j)))
        def _():
            scatter(slot, j).start()

    own = pl.ds(pl.multiple_of(c * ROWS, ROWS), ROWS)

    def kv_part(slot, i, rows):
        ref = kv.at[slot, i // 2, rows, pl.ds((i % 2) * 512, 512)]
        return pltpu.make_async_remote_copy(
            ref, ref, kv_send.at[slot, i], kv_recv.at[slot, i], device_id=partner, device_id_type=MESH
        )

    def kv_copy(slot, i):
        return kv_part(slot, i, own)

    def kv_arrival(slot, i):
        return kv_part(slot, i, pl.ds(pl.multiple_of((1 - c) * ROWS, ROWS), ROWS))

    def hand_over():
        return pltpu.make_async_remote_copy(
            depth, res, hand_send, hand_recv, device_id=partner, device_id_type=MESH
        )

    def rim_copy(slot):
        return pltpu.make_async_remote_copy(
            rim_out.at[slot],
            rim_in.at[slot],
            rim_send.at[slot],
            rim_recv.at[slot],
            device_id=partner,
            device_id_type=MESH,
        )

    def run_slot(slot, carry, fast):
        mine = slot == c

        def wait_for(*ids):
            for i in ids:

                @pl.when(mine)
                def _(i=i):
                    local(i).wait()

                @pl.when(jnp.logical_not(mine))
                def _(i=i):
                    pull(i, slot).wait_recv()

        if fast:
            wait_for(*range(15))

        def ready(*ids):
            if not fast:
                wait_for(*ids)

        length = lengths[u]

        def input_ready(j):
            def remote():
                pltpu.make_async_remote_copy(
                    first_piece, first_piece, x_send.at[0], x_recv.at[j], device_id=partner, device_id_type=MESH
                ).wait_recv()

            if fast:
                remote()
                return
            itself = lead & (j == t) & (t < 4)

            @pl.when(itself)
            def _():
                frame_local(u).wait()

            pl.when(jnp.logical_not(itself))(remote)

        opening = (k == 0) & (slot == 0)
        passes = jnp.where(opening, jnp.where(c == 0, 4, 0), 2)

        def when_opening(condition):
            return pl.when(opening & condition) if not fast else (lambda f: None)

        if not fast:

            @pl.when(jnp.logical_not(opening & (c == 1)))
            def _():
                ready(0, 7, 8)

        def feed_forward(i, carry):
            group = i // 2
            source = xs.at[slot + group]
            rows = pl.ds(i * HALF, HALF) if fast else pl.ds(pl.multiple_of(lax.rem(i, 2) * HALF, HALF), HALF)

            @pl.when(slot == 0)
            def _():
                input_ready(2 * i)
                input_ready(2 * i + 1)

            act[rows] = normed(source[rows].astype(F32), vec[slot, 0]).astype(BF16)
            for n in range(4):
                cols = pl.ds(n * 512, 512)
                v = dot(act[rows], w_up[slot, :, cols])
                wide[rows, cols] = (v * sigmoid(v)).astype(BF16)
            for n in range(2):
                cols = pl.ds(n * 512, 512)
                v = dot(wide[rows], w_down[slot, :, cols])
                sums[group, rows, cols] = source[rows, cols].astype(F32) + 0.5 * v
            return carry

        if not fast:
            lax.fori_loop(0, passes, feed_forward, 0)

        @when_opening(c == 0)
        def _():
            hand_over().start()

        @when_opening(c == 1)
        def _():
            hand_over().wait_recv()

        ready(1, 9, 10)

        def attention_input(rows, offset, length, share):
            act[rows] = normed(res[rows], vec[slot, 1]).astype(BF16)
            mine_rows = pl.ds(pl.multiple_of(c * ROWS + offset, HALF), length)
            for i in range(4):
                cols = pl.ds((i // 2) * 512, 512)
                w = (w_key, w_value)[i % 2]
                kv[slot, i % 2, mine_rows, cols] = dot(act[rows], w[slot, :, cols]).astype(BF16)
                if share:
                    kv_copy(slot, 2 * (i % 2) + i // 2).start()

        if fast:
            for i in range(2):
                feed_forward(i, 0)
        attention_input(pl.ds(0, ROWS), 0, ROWS, True)
        if not fast:
            push_part(1, opening)

        @pl.when(slot == 1)
        def _():
            for j in range(PIECES):
                emit(0, j)

        ready(11)
        for n in range(2):
            cols = pl.ds(n * 512, 512)
            wide[:, cols] = (dot(act[...], w_query[slot, :, cols]) * QUERY_SCALE).astype(BF16)
        kv_arrival(slot, 0).wait_recv()
        kv_arrival(slot, 2).wait_recv()

        low = lax.broadcasted_iota(jnp.int32, (ROWS, 128), 1) < 64
        one = jnp.where(lax.broadcasted_iota(jnp.int32, (ROWS, 128), 1) == 0, 1.0, 0.0).astype(BF16)
        ones = jnp.ones((LEN, 128), BF16)

        def pair_scores(g):
            cols = pl.ds(g * 128, 128)
            q = wide[:, cols]
            none = jnp.zeros_like(q)
            stacked = jnp.concatenate(
                [
                    jnp.concatenate([jnp.where(low, q, none), one], axis=1),
                    jnp.concatenate([jnp.where(low, none, q), one], axis=1),
                ],
                axis=0,
            )
            keys = jnp.concatenate([kv[slot, 0, :, cols], bias[...]], axis=1)
            return lax.dot_general(
                stacked, keys, (((1,), (1,)), ((), ())), preferred_element_type=F32
            )

        def pair_context(g, scores):
            cols = pl.ds(g * 128, 128)
            peak = jnp.max(scores, axis=-1, keepdims=True)
            weights = jnp.exp2(scores - peak).astype(BF16)
            values = jnp.concatenate([kv[slot, 1, :, cols], ones], axis=1)
            mixed = dot(weights, values)
            total = jnp.where(low, mixed[:ROWS, 128:], mixed[ROWS:, 128:])
            mixed = jnp.where(low, mixed[:ROWS, :128], mixed[ROWS:, :128])
            act[:, cols] = (mixed / total).astype(BF16)

        scores = pair_scores(0)
        for g in range(HEADS // 2):
            if g == 3:
                kv_arrival(slot, 1).wait_recv()
                kv_arrival(slot, 3).wait_recv()
            later = pair_scores(g + 1) if g + 1 < HEADS // 2 else None
            pair_context(g, scores)
            scores = later
        ready(12)

        def out_tile(n):
            cols = pl.ds(n * 512, 512)
            res[:, cols] = res[:, cols] + dot(act[...], w_out[slot, :, cols])

        for n in range(2):
            out_tile(n)
        ready(2, 13, 6)

        @when_opening(c == 0)
        def _():
            hand_over().wait_send()

        wide[:, :D] = normed(res[...], vec[slot, 2]).astype(BF16)
        row = c * ROWS + lax.broadcasted_iota(jnp.int32, (ROWS, 256), 0)
        keep = (row < length).astype(F32)

        def glu_tile(n):
            value = dot(wide[:, :D], w_expand[slot, :, pl.ds(n * 256, 256)])
            gate = dot(wide[:, :D], w_expand[slot, :, pl.ds(n * 256 + D, 256)])
            glu = (value * sigmoid(gate) * keep).astype(BF16)
            rim_out[slot, :, pl.ds(n * 256, 256)] = jnp.where(c == 0, glu[ROWS - 16 :], glu[:16])
            glu = glu.astype(F32)
            padded[2 * n, pl.ds(16, ROWS), :] = glu[:, :128]
            padded[2 * n + 1, pl.ds(16, ROWS), :] = glu[:, 128:]

        def conv_rows(n, base, blocks):
            cols = pl.ds(n * 128, 128)
            weights = [taps[slot, j, :, cols] for j in range(TAPS)]
            total = [None] * blocks
            for o in range(1, 8 * (blocks - 1) + TAPS + 1):
                v = padded[n, pl.ds(base + o, 8), :]
                for b in range(blocks):
                    j = o - 1 - 8 * b
                    if 0 <= j < TAPS:
                        term = v * weights[j]
                        total[b] = term if total[b] is None else total[b] + term
            for b in range(blocks):
                depth[pl.ds(base + 8 * b, 8), cols] = total[b]

        for n in range(5):
            if n < 4:
                glu_tile(n)
            if n == 3:
                rim_copy(slot).start()
                if not fast:
                    push_part(2, opening)
            if n > 0:
                for i in (2 * n - 2, 2 * n - 1):
                    conv_rows(i, 0, 16)
                    conv_rows(i, 128, 16)
        ready(3, 4)
        rim_copy(slot).wait_recv()
        inner_rim = pl.ds(pl.multiple_of((1 - c) * (ROWS + 16), 16), 16)
        edge = pl.multiple_of((1 - c) * (ROWS - 16), 16)
        for n in range(8):
            padded[n, inner_rim, :] = rim_in[slot, :, n * 128 : (n + 1) * 128].astype(F32)
            conv_rows(n, edge, 2)
        ready(14, 5)
        for h in range(2):
            rows = pl.ds(h * HALF, HALF)
            shifted = normed(depth[rows], vec[slot, 3]) + vec[slot, 4]
            act[rows] = (shifted * sigmoid(shifted)).astype(BF16)
            closing = res[rows] + dot(act[rows], w_shrink[slot])
            xs[slot + 1, rows] = normed(closing, vec[slot, 5]).astype(BF16)
            for j in (2 * h, 2 * h + 1):

                @pl.when((slot == 1) & (k < STAGES - 1))
                def _(j=j):
                    if j == 0:

                        @pl.when(even)
                        def _():
                            for n in range(PIECE // CHUNK):
                                leave_x(n).start()

                        @pl.when(jnp.logical_not(even))
                        def _():
                            leave_z().start()

                    else:
                        forward(j).start()

                @pl.when((slot == 1) & (k == STAGES - 1))
                def _(j=j):
                    emit(1, j)

        @pl.when((slot == 1) & (k < STAGES - 1))
        def _():
            for j in range(PIECES):
                emit(1, j)

        return carry

    @pl.when(active)
    def _():
        seen = lax.broadcasted_iota(jnp.int32, (LEN, 128), 0) < lengths[u]
        bias[...] = jnp.where(seen, 0.0, -1e30).astype(BF16)
        for n in range(8):
            padded[n, pl.ds(0, 16), :] = jnp.zeros((16, 128), F32)
            padded[n, pl.ds(16 + ROWS, 16), :] = jnp.zeros((16, 128), F32)

        @pl.when(k == 0)
        def _():
            lax.fori_loop(0, 2, functools.partial(run_slot, fast=False), 0)

        @pl.when(k > 0)
        def _():
            lax.fori_loop(0, 2, functools.partial(run_slot, fast=True), 0)

        for i in ORDER:

            @pl.when(pushed(i))
            def _(i=i):
                push(i).wait_send()

        for slot in range(2):
            for i in range(4):
                kv_copy(slot, i).wait_send()
            rim_copy(slot).wait_send()
            for j in range(PIECES):

                @pl.when(jnp.logical_not(own_piece(slot, j)))
                def _(slot=slot, j=j):
                    scatter(slot, j).wait_send()

        @pl.when(k < STAGES - 1)
        def _():
            for j in range(PIECES):
                forward(j).wait_send()

    for v in range(UTTS):

        @pl.when(sends_frames & jnp.logical_not((c == 0) & (t == 2 * v + 1)))
        def _(v=v):
            frame_copy(v).wait_send()

    for v in range(UTTS):
        itself = (t == 2 * v + side) & (c == t // 4)
        landed = out.at[0, v]

        @pl.when(itself)
        def _(v=v, landed=landed):
            pltpu.make_async_copy(xs.at[0, piece_rows(0)], landed, out_recv.at[v]).wait()

        @pl.when(jnp.logical_not(itself))
        def _(v=v, landed=landed):
            pltpu.make_async_remote_copy(
                landed, landed, out_send.at[0, 0], out_recv.at[v], device_id=partner, device_id_type=MESH
            ).wait_recv()


def body(
    frames,
    lengths,
    ffn_gain,
    ffn_up,
    ffn_down,
    attn_gain,
    query_weight,
    key_weight,
    value_weight,
    out_weight,
    conv_gain,
    expand_weight,
    depth_weight,
    depth_gain,
    norm_shift,
    shrink_weight,
    final_gain,
):
    anywhere = pl.BlockSpec(memory_space=pl.ANY)
    dma = pltpu.SemaphoreType.DMA
    return pl.pallas_call(
        block_kernel,
        name="conformer",
        out_shape=jax.ShapeDtypeStruct((1, UTTS, PIECE, D), BF16),
        in_specs=[pl.BlockSpec(memory_space=pltpu.SMEM)] + [anywhere] * 16,
        out_specs=anywhere,
        scratch_shapes=[pltpu.VMEM((2,) + shape, BF16) for shape in SHAPES]
        + [
            pltpu.VMEM((2, 6, 1, D), F32),
            pltpu.VMEM((2, TAPS, 1, D), F32),
            pltpu.VMEM((3, ROWS, D), BF16),
            pltpu.VMEM((ROWS, D), BF16),
            pltpu.VMEM((ROWS, FF), BF16),
            pltpu.VMEM((2, ROWS, D), F32),
            pltpu.VMEM((2, 2, LEN, D), BF16),
            pltpu.VMEM((2, 16, D), BF16),
            pltpu.VMEM((2, 16, D), BF16),
            pltpu.VMEM((LEN, 128), BF16),
            pltpu.VMEM((8, ROWS + 32, 128), F32),
            pltpu.VMEM((PIECE, D), BF16),
            pltpu.VMEM((PIECE, D), BF16),
            dma((15,)),
            dma((15,)),
            dma((15,)),
            dma((PIECES,)),
            dma((2 * PIECES,)),
            dma((2, PIECES)),
            dma((UTTS,)),
            dma((2, 4)),
            dma((2, 4)),
            dma((2,)),
            dma((2,)),
            dma((UTTS,)),
            dma,
            dma,
            dma((PIECE // CHUNK,)),
            dma((PIECE // CHUNK,)),
            dma,
            dma,
        ],
        compiler_params=pltpu.CompilerParams(
            has_side_effects=True, vmem_limit_bytes=67043328
        ),
    )(
        lengths,
        frames,
        ffn_gain,
        attn_gain,
        conv_gain,
        depth_gain,
        norm_shift,
        final_gain,
        jnp.transpose(depth_weight, (1, 0, 2)),
        ffn_up,
        ffn_down,
        key_weight,
        value_weight,
        query_weight,
        out_weight,
        expand_weight,
        shrink_weight,
    )


def solution(mesh):
    return jax.shard_map(
        body,
        mesh=mesh,
        in_specs=(
            P(None, "tm", None),
            P(),
            P("section", None),
            P("section", None, None),
            P("section", None, None),
            P("section", None),
            P("section", None, None),
            P("section", None, None),
            P("section", None, None),
            P("section", None, None),
            P("section", None),
            P("section", None, None),
            P("section", None, None),
            P("section", None),
            P("section", None),
            P("section", None, None),
            P("section", None),
        ),
        out_specs=P("section", None, "tm", None),
        check_vma=False,
    )
```
